256 devices in a mesh: rows: 64 (over z, x, core), grp: 4 (over y).
Axes of the slice: x: 4, y: 4, z: 8, core: 2. Of those that a mesh axis runs over, the one named last changes fastest.
Arguments:
- user_features: bfloat16 [4, 16384, 256], P('grp', 'rows'), may hold values from -72 to 72
- w_first: bfloat16 [256, 256], replicated, may hold values from -0.375 to 0.375
- w_second: bfloat16 [256, 256], replicated, may hold values from -0.375 to 0.375
- item_embed: bfloat16 [4, 16384, 256], P('grp', 'rows'), may hold values from -27 to 27
- example_weight: float32 [4, 16384], P('grp', 'rows'), may hold values from 0.02 to 0.2
- positive: int32 [4, 16384], P('grp', 'rows'), may hold values from 0 to 16383
- item_owner: int32 [4, 16384, 1], P('grp', 'rows'), may hold values from 0 to 63; in each aligned block of 256 rows (0 to 255, 256 to 511, ..., all dimensions but the last counted through in order) at most 16 rows name the same one
- item_row: int32 [4, 16384], P('grp', 'rows'), may hold values from 0 to 4095
Outputs:
- grad_first: float32 [256, 256], replicated
- grad_second: float32 [256, 256], replicated
- grad_table: float32 [262144, 256], P('rows', 'grp')
The draws below stay inside these ranges and needn't reach their ends.
Inputs may be any that keep to these rules, and one draw needn't show every extreme that they name: `item_owner`: within the rows of one device (aligned blocks of 256 pairs of a group) no owner is named by more than 16 pairs, a bound that some block reaches.
All inputs are finite; a program needn't handle non-finite values.
Results may differ from the reference program's by a relative error of at most 0.0023.
The reference program's roundings to bfloat16 on the way count: a program that leaves them out, or rounds other values in their place, can miss the bound.
Values may be sent and summed in bfloat16 or wider, within the bound.
No kernel may reach another device: no remote copies, remote signals or barrier semaphores. Data moves between devices by JAX's collectives and lax.ppermute only.
A program may use at most 128 MiB of HBM per device.

```python
import math
import jax
import jax.numpy as jnp
import numpy as np
from jax import lax

D = 256
DIN = 256
DH = 256
BATCH_DEV = 256
ITEMS_DEV = 4096
GU = 16384
CAP = 16
N_ROWS = 64
N_GRP = 4


def draw_user_features(key, part):
    first_key = jax.random.fold_in(jax.random.fold_in(key, 11), 0)
    values = jnp.clip(jax.random.normal(first_key, (N_GRP, GU, DIN), jnp.float32), -6.0, 6.0)
    return values.astype(jnp.bfloat16)


def draw_item_embed(key, part):
    first_key = jax.random.fold_in(jax.random.fold_in(key, 23), 0)
    values = 0.15 * jnp.clip(jax.random.normal(first_key, (N_GRP, GU, D), jnp.float32), -6.0, 6.0)
    return values.astype(jnp.bfloat16)


def with_ends(entries, own_key, least, top_value):
    dims = entries.shape
    place = [jax.random.randint(jax.random.fold_in(own_key, axis), (), 0, dims[axis]) for axis in range(len(dims))]
    entries = entries.at[tuple(place)].set(least)
    longest = dims.index(max(dims))
    place[longest] = (place[longest] + 1) % dims[longest]
    return entries.at[tuple(place)].set(top_value)


def shard_levels(rng, dims, shards, low, largest):
    gain = 1.0
    for axis_at, shards_of in shards:
        draws = jax.random.uniform(jax.random.fold_in(jax.random.fold_in(rng, 6), axis_at), (shards_of,), jnp.float32, low / len(shards), largest / len(shards))
        gain = gain * jnp.repeat(jnp.exp(draws), dims[axis_at] // shards_of).reshape((-1,) + (1,) * (len(dims) - 1 - axis_at))
    return gain


def cumulative_ranks(number_of, slope):
    loads = [(1 << 20) // math.isqrt(standing ** slope) + 1 for standing in range(1, number_of + 1)]
    width = 1 + sum(loads) // (1 << 30)
    return np.cumsum(np.array([max(1, weight // width) for weight in loads]))


def ranked_ids(own_key, extent, amount, lean):
    listing = cumulative_ranks(amount, lean)
    pick = jax.random.randint(jax.random.fold_in(own_key, 1), extent, 0, int(listing[amount - 1]))
    standing = jnp.searchsorted(jnp.asarray(listing, jnp.int32), pick, side="right")
    return jax.random.permutation(jax.random.fold_in(own_key, 2), amount)[standing].astype(jnp.int32)


def assign_block(rng, own, number, rows, count, top, limit, skew):
    ranking = jax.random.permutation(rng, count)
    packed, common = shares(count, rows * top, limit, skew, True), shares(count, rows * top, limit, skew, False)
    places = jnp.arange(count)

    def named(tallies, rotation):
        used = int((tallies > 0).sum())
        fixed = max(1, used // 4)
        passed = fixed + (places - fixed + rotation * (used - fixed)) % max(1, count - fixed)
        return jnp.zeros((count,), jnp.int32).at[ranking[jnp.where(places < fixed, places, passed)]].set(jnp.asarray(tallies, jnp.int32))

    tallies = jnp.where(number % 4 == 0, named(packed, number // 4), named(common, number - number // 4 - 1))
    mixed = jax.random.permutation(jax.random.fold_in(own, 3), count)
    donor, sink = mixed[0:count // 2 * 2:2], mixed[1:count // 2 * 2:2]
    room = jnp.minimum(tallies[donor] - 1, limit - tallies[sink]) // 2
    room = jnp.where((donor == ranking[0]) | (sink == ranking[0]) | (tallies[sink] == 0), 0, jnp.maximum(room, 0))
    passed = jax.random.randint(jax.random.fold_in(own, 4), (count // 2,), 0, 1 << 20) % (room + 1)
    tallies = tallies.at[donor].add(-passed).at[sink].add(passed)
    labels = jnp.searchsorted(jnp.cumsum(tallies), jnp.arange(rows * top), side="right").astype(jnp.int32)
    grid = labels.reshape(top, rows).T
    grid = grid[jax.random.permutation(jax.random.fold_in(own, 1), rows)]
    rotation = jax.random.randint(jax.random.fold_in(own, 2), (rows, 1), 0, top)
    return jnp.take_along_axis(grid, (jnp.arange(top)[None, :] + rotation) % top, axis=1)


def shares(amount, total, reach, skew, full):
    portions = [(1 << 20) // math.isqrt(grade ** skew) + 1 for grade in range(1, amount + 1)]
    largest = reach if full else min(reach, max(-(-total // amount), total * portions[0] // sum(portions)))
    least = 1 if total - largest >= amount - 1 else 0
    counts, surplus = [largest] + [least] * (amount - 1), total - largest - least * (amount - 1)
    while surplus > 0:
        candidates = [i for i in range(1, amount) if counts[i] < largest] or [i for i in range(1, amount) if counts[i] < reach]
        pool, remaining = sum([portions[i] for i in candidates]), surplus
        for i in candidates:
            more = min(reach - counts[i], max(1, remaining * portions[i] // pool), surplus)
            counts[i] = counts[i] + more
            surplus = surplus - more
    return np.array(counts)


def centred(rng, dims, scale, reach, held_as=jnp.bfloat16):
    array = scale * jax.random.normal(rng, dims, jnp.float32)
    return jnp.clip(array, min=-reach, max=reach).astype(held_as)


def setup_inputs(seed: int = 0) -> dict:
    key_list = jax.random.split(jax.random.key(seed), 9)
    user_features = draw_user_features(jax.random.fold_in(key_list[8], 71), 0)
    w_first = centred(key_list[1], (DIN, DH), DIN ** -0.5, 0.375)
    w_second = centred(key_list[2], (DH, D), DH ** -0.5, 0.375)
    item_embed = draw_item_embed(jax.random.fold_in(key_list[8], 71), 0)
    example_weight = jnp.clip(jnp.exp(math.log(0.2) - 2.3025851 * jax.random.uniform(key_list[4], (N_GRP, GU), jnp.float32) ** shard_levels(key_list[4], (N_GRP, GU), ((0, 4), (1, 64)), -0.2, 0.2)), 0.02, 0.2)
    positive = with_ends(jax.random.randint(key_list[5], (N_GRP, GU), 0, GU), jax.random.fold_in(key_list[5], 1), 0, GU - 1).astype(jnp.int32)
    item_owner_keys = jax.random.split(jax.random.fold_in(key_list[6], 1), N_GRP * GU // BATCH_DEV)
    item_owner_turns = jax.random.permutation(jax.random.fold_in(key_list[6], 3), N_GRP * GU // BATCH_DEV)
    item_owner = jax.vmap(lambda own, number: assign_block(jax.random.fold_in(key_list[6], 2), own, number, BATCH_DEV, N_ROWS, 1, CAP, 2))(item_owner_keys, item_owner_turns).reshape((N_GRP, GU, 1))
    item_row = with_ends(ranked_ids(key_list[7], (N_GRP, GU), ITEMS_DEV, 2), jax.random.fold_in(key_list[7], 3), 0, ITEMS_DEV - 1).astype(jnp.int32)
    return dict(user_features=user_features, w_first=w_first, w_second=w_second, item_embed=item_embed, example_weight=example_weight, positive=positive, item_owner=item_owner, item_row=item_row)


def reference(user_features, w_first, w_second, item_embed, example_weight, positive, item_owner, item_row):
    group_users = user_features.shape[1]
    row_block = math.gcd(group_users, 1024)
    num_blocks = group_users // row_block

    def one_group(inputs):
        features, group_items, weights, targets = inputs
        pre_act = jnp.dot(features, w_first, preferred_element_type=jnp.float32)
        hidden = jax.nn.silu(pre_act).astype(jnp.bfloat16)
        user_vecs = jnp.dot(hidden, w_second, preferred_element_type=jnp.float32).astype(jnp.bfloat16)
        items_wide = group_items.astype(jnp.float32)
        users_wide = user_vecs.astype(jnp.float32)
        columns = jnp.arange(group_users, dtype=jnp.int32)

        def block_step(accum, block_no):
            first_row = (block_no * row_block).astype(jnp.int32)
            user_block = lax.dynamic_slice_in_dim(users_wide, first_row, row_block, 0)
            weight_block = lax.dynamic_slice_in_dim(weights, first_row, row_block, 0)
            target_block = lax.dynamic_slice_in_dim(targets, first_row, row_block, 0)
            scores = jnp.dot(user_block, items_wide.T)
            row_max = jnp.max(scores, axis=1, keepdims=True)
            log_total = row_max + jnp.log(jnp.sum(jnp.exp(scores - row_max), axis=1, keepdims=True))
            chosen = (columns[None, :] == target_block[:, None]).astype(jnp.float32)
            dscore = (weight_block[:, None] * (jnp.exp(scores - log_total) - chosen)).astype(jnp.bfloat16)
            dscore_wide = dscore.astype(jnp.float32)
            grad_block = jnp.dot(dscore_wide, items_wide)
            accum = accum + jnp.dot(dscore_wide.T, user_block)
            return accum, grad_block

        grad_item, grad_blocks = lax.scan(block_step, jnp.zeros((group_users, D), jnp.float32),
                                          jnp.arange(num_blocks, dtype=jnp.int32))
        grad_user = grad_blocks.reshape(group_users, D).astype(jnp.bfloat16)
        d_second = jnp.dot(hidden.T, grad_user, preferred_element_type=jnp.float32)
        back_grad = jnp.dot(grad_user, w_second.T, preferred_element_type=jnp.float32)
        sigmoid_pre = jax.nn.sigmoid(pre_act)
        grad_pre = (back_grad * sigmoid_pre * (1.0 + pre_act * (1.0 - sigmoid_pre))).astype(jnp.bfloat16)
        d_first = jnp.dot(features.T, grad_pre, preferred_element_type=jnp.float32)
        return grad_item, d_first, d_second

    grad_item, d_first, d_second = lax.map(one_group, (user_features, item_embed, example_weight, positive))
    grad_first = jnp.sum(d_first, axis=0)
    grad_second = jnp.sum(d_second, axis=0)
    table_ids = (item_owner[:, :, 0] * ITEMS_DEV + item_row).astype(jnp.int32)
    grad_table = jax.ops.segment_sum(grad_item.reshape(-1, D), table_ids.reshape(-1),
                                     num_segments=ITEMS_DEV * N_ROWS)
    return grad_first, grad_second, grad_table
```

```python
import jax
import jax.numpy as jnp
from jax import lax
from jax.experimental import pallas as pl
from jax.experimental.pallas import tpu as pltpu
from jax.sharding import Mesh
from jax.sharding import PartitionSpec as P

TABLE = 4096
CAP = 16
BLK = 256
XK = ("x", "k")
XKY = ("x", "k", "y")
ALL = ("z", "x", "k", "y")
F32 = jnp.float32
BF16 = jnp.bfloat16


def dot(left, right, dims):
    return lax.dot_general(left, right, ((dims[0:1], dims[1:2]), ((), ())), preferred_element_type=F32)


def exchange(value, axes):
    return lax.all_to_all(value, axes, 0, 0, tiled=True)


def to_all(value, axes):
    return exchange(jnp.broadcast_to(value[None], (lax.axis_size(axes), *value.shape)), axes)


def stats_kernel(items_ref, users_ref, own_ref, out_ref):
    rows = []
    sums = []
    for c in range(8):
        scores = dot(items_ref[...], users_ref[c * BLK : (c + 1) * BLK, :], (1, 1))
        top = jnp.max(scores, axis=0, keepdims=True)
        rows.append(top)
        sums.append(jnp.sum(jnp.exp(scores - top), axis=0, keepdims=True))
    chunk = jnp.concatenate(rows + sums + [own_ref[...]], axis=0)
    for p in range(8):
        out_ref[p] = chunk


def stats(items, users, own):
    return pl.pallas_call(
        stats_kernel,
        out_shape=jax.ShapeDtypeStruct((8, 24, BLK), F32),
        compiler_params=pltpu.CompilerParams(vmem_limit_bytes=56 * 2**20),
        name="stats",
    )(items, users, own)


def grads_kernel(base_ref, items_ref, turned_ref, users_ref, got_ref, gi_ref, gu_ref, acc_ref):
    shard = 8 * BLK
    place = lax.broadcasted_iota(jnp.int32, (shard, BLK), 0)
    index = (place // BLK) * shard + base_ref[0] + (place % BLK)
    for c in range(8):
        tops = got_ref[:, c, :]
        parts = got_ref[:, 8 + c, :]
        top = jnp.max(tops, axis=0, keepdims=True)
        total = top + jnp.log(jnp.sum(parts * jnp.exp(tops - top), axis=0, keepdims=True))
        weight = got_ref[c, 16:17, :]
        target = got_ref[c, 17:18, :].astype(jnp.int32)
        users = users_ref[c * BLK : (c + 1) * BLK, :]
        scores = dot(items_ref[...], users, (1, 1))
        chosen = (index == target).astype(F32)
        dscore = (weight * (jnp.exp(scores - total) - chosen)).astype(BF16)
        gu_ref[c] = dot(turned_ref[...], dscore, (1, 0))
        part = dot(dscore, users, (1, 0))
        if c == 0:
            acc_ref[...] = part
        elif c < 7:
            acc_ref[...] += part
        else:
            gi_ref[...] = (acc_ref[...] + part).astype(BF16)


def grads(base, items, turned, users, got):
    vmem = pl.BlockSpec(memory_space=pltpu.VMEM)
    return pl.pallas_call(
        grads_kernel,
        in_specs=[pl.BlockSpec(memory_space=pltpu.SMEM), vmem, vmem, vmem, vmem],
        out_shape=(
            jax.ShapeDtypeStruct((8 * BLK, 256), BF16),
            jax.ShapeDtypeStruct((8, 256, BLK), F32),
        ),
        scratch_shapes=[pltpu.VMEM((8 * BLK, 256), F32)],
        compiler_params=pltpu.CompilerParams(vmem_limit_bytes=56 * 2**20),
        name="grads",
    )(base, items, turned, users, got)


def thirds(value):
    high = value.astype(BF16)
    rest = value - high.astype(F32)
    middle = rest.astype(BF16)
    return high, middle, (rest - middle.astype(F32)).astype(BF16)


def pack_kernel(parts_ref, owner_ref, rank_ref, out_ref):
    value = jnp.sum(parts_ref[...].astype(F32), axis=0)
    pieces = thirds(value)
    lane = lax.broadcasted_iota(jnp.int32, (64 * 8, BLK), 0)
    halves = []
    for h in range(2):
        rank = rank_ref[...] - 8 * h
        slot = jnp.where((rank >= 0) & (rank < 8), owner_ref[...] * 8 + rank, -1)
        pick = (lane == slot).astype(F32).astype(BF16)
        halves.append(sum(dot(pick, piece, (1, 0)) for piece in pieces))
    for g in range(4):
        share = slice(64 * g, 64 * g + 64)
        both = jnp.concatenate([halves[0][:, share], halves[1][:, share]], axis=1)
        out_ref[:, g] = both.reshape(64, 8, 128)


def pack(parts, owner, rank):
    return pl.pallas_call(
        pack_kernel, out_shape=jax.ShapeDtypeStruct((64, 4, 8, 128), F32), name="pack"
    )(parts, owner, rank)


def table_kernel(got_ref, ids_ref, out_ref):
    both = got_ref[...].T
    value = jnp.concatenate([both[:64], both[64:]], axis=1)
    pieces = jnp.concatenate(thirds(value), axis=0)
    ids = ids_ref[...]
    upper = ids >> 8
    lower = ids & 255
    pick = (lax.broadcasted_iota(jnp.int32, (256, TABLE), 0) == lower).astype(F32).astype(BF16)
    zero = jnp.zeros((), BF16)
    for a in range(16):
        keep = jnp.broadcast_to((upper == a).astype(F32), (16, TABLE)).astype(BF16)
        kept = pieces * jnp.concatenate([keep] * 12, axis=0)
        part = dot(kept, pick, (1, 1))
        out_ref[:, a * 256 : (a + 1) * 256] = part[:64] + part[64:128] + part[128:]


def table(got, ids):
    return pl.pallas_call(
        table_kernel,
        out_shape=jax.ShapeDtypeStruct((64, TABLE), F32),
        compiler_params=pltpu.CompilerParams(vmem_limit_bytes=56 * 2**20),
        name="table",
    )(got, ids)


def tower(features, w_first, w_second):
    pre_act = jnp.dot(features, w_first, preferred_element_type=F32)
    hidden = jax.nn.silu(pre_act).astype(BF16)
    return pre_act, hidden, jnp.dot(hidden, w_second, preferred_element_type=F32).astype(BF16)


def body(user_features, w_first, w_second, item_embed, example_weight, positive, item_owner, item_row):
    features = user_features[0]
    owner = item_owner.reshape(1, BLK)
    items = to_all(item_embed[0], "z").reshape(8 * BLK, 256)
    block = to_all(features, XK).reshape(8 * BLK, 256)
    _, _, users = tower(block, w_first, w_second)

    member = (owner == lax.broadcasted_iota(jnp.int32, (64, 1), 0)).astype(F32)
    order = lax.broadcasted_iota(jnp.int32, (BLK, BLK), 0) < lax.broadcasted_iota(jnp.int32, (BLK, BLK), 1)
    before = dot(member.astype(BF16), order.astype(BF16), (1, 0))
    rank = jnp.sum(before * member, axis=0, keepdims=True).astype(jnp.int32)
    slot = owner * CAP + rank
    held = (slot == lax.broadcasted_iota(jnp.int32, (64 * CAP, 1), 0)).astype(jnp.int32)
    rows = jnp.sum(held * (item_row + 1), axis=1) - 1
    rows = jnp.broadcast_to(rows.reshape(64, 1, CAP), (64, 4, CAP)).reshape(256, CAP)
    ids = exchange(rows, ALL)
    ids = jnp.concatenate([ids[:, :8].reshape(1, -1), ids[:, 8:].reshape(1, -1)], axis=1)

    own = jnp.concatenate(
        [example_weight, positive.astype(F32), jnp.zeros((6, BLK), F32)], axis=0
    )
    got = exchange(stats(items, users, own), XK)
    base = (lax.axis_index(XK) * BLK).astype(jnp.int32).reshape(1)
    gi, gu = grads(base, items, items.T, users, got)
    gi = exchange(gi.reshape(8, BLK, 256), "z")
    gu = exchange(gu, XK)

    send = pack(gi, owner, rank).reshape(256, 8, 128)
    came = exchange(send, ALL).reshape(256 * 8, 128)
    grad_table = table(came, ids).T

    pre_act, hidden, _ = tower(features, w_first, w_second)
    grad_user = jnp.sum(gu, axis=0).T.astype(BF16)
    d_second = dot(hidden, grad_user, (0, 0))
    back_grad = dot(grad_user, w_second, (1, 1))
    gate = jax.nn.sigmoid(pre_act)
    grad_pre = (back_grad * gate * (1.0 + pre_act * (1.0 - gate))).astype(BF16)
    d_first = dot(features, grad_pre, (0, 0))
    both = jnp.concatenate([d_first, d_second], axis=0).reshape(32, 16, 256)
    both = jnp.sum(exchange(both, XKY), axis=0)
    both = jnp.sum(to_all(both, "z"), axis=0)
    both = to_all(both, XKY).reshape(512, 256)
    return both[:256], both[256:], grad_table


def solution(mesh):
    torus = Mesh(mesh.devices.reshape(8, 4, 2, mesh.shape["grp"]), ("z", "x", "k", "y"))
    rows = ("z", "x", "k")
    placed = (
        P("y", rows, None),
        P(),
        P(),
        P("y", rows, None),
        P("y", rows),
        P("y", rows),
        P("y", rows, None),
        P("y", rows),
    )
    return jax.shard_map(
        body, mesh=torus, in_specs=placed, out_specs=(P(), P(), P(rows, "y")), check_vma=False
    )
```

```python
import jax
import jax.numpy as jnp
from jax import lax
from jax.experimental import pallas as pl
from jax.experimental.pallas import tpu as pltpu
from jax.sharding import Mesh
from jax.sharding import PartitionSpec as P

TABLE = 4096
CAP = 16
BLK = 256
XK = ("x", "k")
ZXK = ("z", "x", "k")
YZXK = ("y", "z", "x", "k")
F32 = jnp.float32
BF16 = jnp.bfloat16


def dot(left, right, dims):
    return lax.dot_general(left, right, ((dims[0:1], dims[1:2]), ((), ())), preferred_element_type=F32)


def exchange(value, axes):
    return lax.all_to_all(value, axes, 0, 0, tiled=True)


def to_all(value, axes):
    return exchange(jnp.broadcast_to(value[None], (lax.axis_size(axes), *value.shape)), axes)


def shifted(value, axis, step):
    count = lax.axis_size(axis)
    return lax.ppermute(value, axis, [(i, (i + step) % count) for i in range(count)])


def rotated(value, axis):
    return [value] + [shifted(value, axis, d) for d in range(1, lax.axis_size(axis))]


def place(axis, step=0):
    return (lax.axis_index(axis).astype(jnp.uint32) + jnp.uint32(step)) & jnp.uint32(lax.axis_size(axis) - 1)


def rows_at(value, start, count):
    zero = jnp.uint32(0)
    return lax.dynamic_slice(value, (start,) + (zero,) * (value.ndim - 1), (count, *value.shape[1:]))


def summed_share(value, axis):
    count = lax.axis_size(axis)
    rows = value.shape[0] // count
    total = rows_at(value, place(axis) * jnp.uint32(rows), rows)
    for d in range(1, count):
        total = total + shifted(rows_at(value, place(axis, d) * jnp.uint32(rows), rows), axis, d)
    return total


def joined(value, axis):
    count = lax.axis_size(axis)
    tiles = rotated(value, axis)
    rising = [tiles[-d % count] for d in range(count)]
    rows = value.shape[0]
    start = (jnp.uint32(count) - place(axis)) * jnp.uint32(rows)
    return rows_at(jnp.concatenate(rising + rising, axis=0), start, count * rows)


def stats_kernel(*refs):
    *item_refs, users_ref, own_ref, out_ref, items_ref = refs
    for d in range(8):
        items_ref[d * BLK : (d + 1) * BLK, :] = item_refs[d][...]

    def step(c, carry):
        scores = dot(items_ref[...], users_ref[pl.ds(c * BLK, BLK), :], (1, 1))
        top = jnp.max(scores, axis=0, keepdims=True)
        out_ref[0, pl.ds(c, 1), :] = top
        out_ref[0, pl.ds(8 + c, 1), :] = jnp.sum(jnp.exp(scores - top), axis=0, keepdims=True)
        return carry

    lax.fori_loop(0, 8, step, 0)
    out_ref[0, 16:24, :] = own_ref[...]
    for p in range(1, 8):
        out_ref[p] = out_ref[0]


def stats(items, users, own):
    return pl.pallas_call(
        stats_kernel,
        out_shape=jax.ShapeDtypeStruct((8, 24, BLK), F32),
        scratch_shapes=[pltpu.VMEM((8 * BLK, 256), BF16)],
        compiler_params=pltpu.CompilerParams(vmem_limit_bytes=56 * 2**20),
        name="stats",
    )(*items, users, own)


def grads_kernel(base_ref, *refs):
    *item_refs, users_ref, got_ref = refs[:10]
    *gi_refs, gu_ref, acc_ref, items_ref, turned_ref, index_ref = refs[10:]
    place = lax.broadcasted_iota(jnp.int32, (BLK, BLK), 0)
    for d in range(8):
        rows = slice(d * BLK, (d + 1) * BLK)
        items_ref[rows, :] = item_refs[d][...]
        turned_ref[:, rows] = item_refs[d][...].T
        index_ref[rows, :] = place + base_ref[d]
    acc_ref[...] = jnp.zeros_like(acc_ref)

    def step(c, carry):
        tops = got_ref[:, pl.ds(c, 1), :].reshape(8, BLK)
        parts = got_ref[:, pl.ds(8 + c, 1), :].reshape(8, BLK)
        top = jnp.max(tops, axis=0, keepdims=True)
        total = top + jnp.log(jnp.sum(parts * jnp.exp(tops - top), axis=0, keepdims=True))
        weight = got_ref[c, 16:17, :]
        target = got_ref[c, 17:18, :].astype(jnp.int32)
        users = users_ref[pl.ds(c * BLK, BLK), :]
        scores = dot(items_ref[...], users, (1, 1))
        chosen = (index_ref[...] == target).astype(F32)
        dscore = (weight * (jnp.exp(scores - total) - chosen)).astype(BF16)
        gu_ref[c] = dot(turned_ref[...], dscore, (1, 0))
        acc_ref[...] += dot(dscore, users, (1, 0))
        return carry

    lax.fori_loop(0, 8, step, 0)
    for d in range(8):
        part = acc_ref[d * BLK : (d + 1) * BLK, :]
        gi_refs[d][...] = part.astype(gi_refs[d].dtype)


def grads(base, items, users, got):
    vmem = pl.BlockSpec(memory_space=pltpu.VMEM)
    return pl.pallas_call(
        grads_kernel,
        in_specs=[pl.BlockSpec(memory_space=pltpu.SMEM)] + [vmem] * 10,
        out_shape=[jax.ShapeDtypeStruct((BLK, 256), F32 if d == 0 else BF16) for d in range(8)]
        + [jax.ShapeDtypeStruct((8, 256, BLK), F32)],
        scratch_shapes=[
            pltpu.VMEM((8 * BLK, 256), F32),
            pltpu.VMEM((8 * BLK, 256), BF16),
            pltpu.VMEM((256, 8 * BLK), BF16),
            pltpu.VMEM((8 * BLK, BLK), jnp.int32),
        ],
        compiler_params=pltpu.CompilerParams(vmem_limit_bytes=56 * 2**20),
        name="grads",
    )(base, *items, users, got)


def thirds(value):
    high = value.astype(BF16)
    rest = value - high.astype(F32)
    middle = rest.astype(BF16)
    return high, middle, (rest - middle.astype(F32)).astype(BF16)


def pack_kernel(*refs):
    *part_refs, owner_ref, rank_ref, out_ref = refs
    value = sum(ref[...].astype(F32) for ref in part_refs)
    pieces = thirds(value)
    lane = lax.broadcasted_iota(jnp.int32, (64 * 8, BLK), 0)
    halves = []
    for h in range(2):
        rank = rank_ref[...] - 8 * h
        slot = jnp.where((rank >= 0) & (rank < 8), owner_ref[...] * 8 + rank, -1)
        pick = (lane == slot).astype(F32).astype(BF16)
        halves.append(sum(dot(pick, piece, (1, 0)) for piece in pieces))
    for g in range(4):
        share = slice(64 * g, 64 * g + 64)
        both = jnp.concatenate([halves[0][:, share], halves[1][:, share]], axis=1)
        out_ref[g] = both.reshape(64, 8, 128)


def pack(parts, owner, rank):
    return pl.pallas_call(
        pack_kernel, out_shape=jax.ShapeDtypeStruct((4, 64, 8, 128), F32), name="pack"
    )(*parts, owner, rank)


def table_kernel(got_ref, ids_ref, out_ref):
    both = got_ref[...].T
    value = jnp.concatenate([both[:64], both[64:]], axis=1)
    pieces = jnp.concatenate(thirds(value), axis=0)
    ids = ids_ref[...]
    upper = ids >> 8
    lower = ids & 255
    pick = (lax.broadcasted_iota(jnp.int32, (256, TABLE), 0) == lower).astype(F32).astype(BF16)

    def step(a, carry):
        keep = jnp.broadcast_to((upper == a).astype(F32), (16, TABLE)).astype(BF16)
        kept = pieces * jnp.concatenate([keep] * 12, axis=0)
        part = dot(kept, pick, (1, 1))
        at = pl.multiple_of(a * 256, 256)
        out_ref[:, pl.ds(at, 256)] = part[:64] + part[64:128] + part[128:]
        return carry

    lax.fori_loop(0, 16, step, 0)


def table(got, ids):
    return pl.pallas_call(
        table_kernel,
        out_shape=jax.ShapeDtypeStruct((64, TABLE), F32),
        compiler_params=pltpu.CompilerParams(vmem_limit_bytes=56 * 2**20),
        name="table",
    )(got, ids)


def tower(features, w_first, w_second):
    pre_act = jnp.dot(features, w_first, preferred_element_type=F32)
    hidden = jax.nn.silu(pre_act).astype(BF16)
    return pre_act, hidden, jnp.dot(hidden, w_second, preferred_element_type=F32).astype(BF16)


def step_body(
    user_features, w_first, w_second, item_embed, example_weight, positive, item_owner, item_row
):
    features = user_features[0]
    owner = item_owner.reshape(1, BLK)
    items = rotated(item_embed[0], "z")
    block = to_all(features, XK).reshape(8 * BLK, 256)
    _, _, users = tower(block, w_first, w_second)

    member = (owner == lax.broadcasted_iota(jnp.int32, (64, 1), 0)).astype(F32)
    order = lax.broadcasted_iota(jnp.int32, (BLK, BLK), 0) < lax.broadcasted_iota(jnp.int32, (BLK, BLK), 1)
    before = dot(member.astype(BF16), order.astype(BF16), (1, 0))
    rank = jnp.sum(before * member, axis=0, keepdims=True).astype(jnp.int32)
    slot = owner * CAP + rank
    held = (slot == lax.broadcasted_iota(jnp.int32, (64 * CAP, 1), 0)).astype(jnp.int32)
    rows = jnp.sum(held * (item_row + 1), axis=1) - 1
    ids = exchange(rows.reshape(64, CAP), ZXK)
    ids = joined(ids, "y")
    ids = jnp.concatenate([ids[:, :8].reshape(1, -1), ids[:, 8:].reshape(1, -1)], axis=1)

    own = jnp.concatenate(
        [example_weight, positive.astype(F32), jnp.zeros((6, BLK), F32)], axis=0
    )
    got = exchange(stats(items, users, own), XK)
    source = (lax.axis_index("z") - jnp.arange(8)) % 8
    base = (source * 8 * BLK + lax.axis_index(XK) * BLK).astype(jnp.int32)
    *gi, gu = grads(base, items, users, got)
    gi = [gi[0]] + [shifted(gi[d], "z", -d) for d in range(1, 8)]
    gu = exchange(gu, XK)

    send = pack(gi, owner, rank).reshape(256, 8, 128)
    came = exchange(send, YZXK).reshape(256 * 8, 128)
    grad_table = table(came, ids).T

    pre_act, hidden, _ = tower(features, w_first, w_second)
    grad_user = jnp.sum(gu, axis=0).T.astype(BF16)
    d_second = dot(hidden, grad_user, (0, 0))
    back_grad = dot(grad_user, w_second, (1, 1))
    gate = jax.nn.sigmoid(pre_act)
    grad_pre = (back_grad * gate * (1.0 + pre_act * (1.0 - gate))).astype(BF16)
    d_first = dot(features, grad_pre, (0, 0))
    both = jnp.concatenate([d_first, d_second], axis=0)
    for axis in ("k", "y", "x"):
        both = summed_share(both, axis)
    for step in (1, 2, 4):
        both = both + lax.ppermute(both, "z", [(i, i ^ step) for i in range(8)])
    for axis in ("x", "y", "k"):
        both = joined(both, axis)
    return both[:256], both[256:], grad_table


def solution(mesh):
    torus = Mesh(mesh.devices.reshape(8, 4, 2, mesh.shape["grp"]), ("z", "x", "k", "y"))
    rows = ("z", "x", "k")
    placed = (
        P("y", rows, None),
        P(),
        P(),
        P("y", rows, None),
        P("y", rows),
        P("y", rows),
        P("y", rows, None),
        P("y", rows),
    )
    return jax.shard_map(
        step_body, mesh=torus, in_specs=placed, out_specs=(P(), P(), P(rows, "y")), check_vma=False
    )
```

```python
import jax
import jax.numpy as jnp
from jax import lax
from jax.experimental import pallas as pl
from jax.experimental.pallas import tpu as pltpu
from jax.sharding import Mesh
from jax.sharding import PartitionSpec as P

TABLE = 4096
CAP = 16
BLK = 256
ROWS = 8 * BLK
XK = ("x", "k")
KYX = ("k", "y", "x")
ZXK = ("z", "x", "k")
YZXK = ("y", "z", "x", "k")
F32 = jnp.float32
BF16 = jnp.bfloat16
VMEM = pl.BlockSpec(memory_space=pltpu.VMEM)
SMEM = pl.BlockSpec(memory_space=pltpu.SMEM)
PARAMS = pltpu.CompilerParams(vmem_limit_bytes=56 * 2**20)


def dot(left, right, dims):
    return lax.dot_general(left, right, ((dims[0:1], dims[1:2]), ((), ())), preferred_element_type=F32)


def exchange(value, axes):
    return lax.all_to_all(value, axes, 0, 0, tiled=True)


def to_all(value, axes):
    return exchange(jnp.broadcast_to(value[None], (lax.axis_size(axes), *value.shape)), axes)


def shifted(value, axis, step):
    count = lax.axis_size(axis)
    return lax.ppermute(value, axis, [(i, (i + step) % count) for i in range(count)])


def place(axis, step=0):
    return (lax.axis_index(axis).astype(jnp.uint32) + jnp.uint32(step)) & jnp.uint32(lax.axis_size(axis) - 1)


def rows_at(value, start, count):
    zero = jnp.uint32(0)
    return lax.dynamic_slice(value, (start,) + (zero,) * (value.ndim - 1), (count, *value.shape[1:]))


def summed_share(value, axis):
    count = lax.axis_size(axis)
    rows = value.shape[0] // count
    total = rows_at(value, place(axis) * jnp.uint32(rows), rows)
    for d in range(1, count):
        total = total + shifted(rows_at(value, place(axis, d) * jnp.uint32(rows), rows), axis, d)
    return total


def joined(value, axis):
    count = lax.axis_size(axis)
    tiles = [value] + [shifted(value, axis, d) for d in range(1, count)]
    rising = [tiles[-d % count] for d in range(count)]
    rows = value.shape[0]
    start = (jnp.uint32(count) - place(axis)) * jnp.uint32(rows)
    return rows_at(jnp.concatenate(rising + rising, axis=0), start, count * rows)


def stats_kernel(at_ref, items_ref, users_ref, own_ref, out_ref, even_ref, odd_ref):
    def score(c, buffer):
        users = users_ref[pl.ds(pl.multiple_of(at_ref[c], BLK), BLK), :]
        buffer[...] = dot(items_ref[...], users, (1, 1))

    def reduce(c, buffer):
        top = jnp.max(buffer[...], axis=0, keepdims=True)
        out_ref[0, pl.ds(c, 1), :] = top
        out_ref[0, pl.ds(8 + c, 1), :] = jnp.sum(jnp.exp(buffer[...] - top), axis=0, keepdims=True)

    score(0, even_ref)

    def step(i, carry):
        score(2 * i + 1, odd_ref)
        reduce(2 * i, even_ref)
        score(jnp.minimum(2 * i + 2, 7), even_ref)
        reduce(2 * i + 1, odd_ref)
        return carry

    lax.fori_loop(0, 4, step, 0)
    out_ref[0, 16:24, :] = own_ref[...]
    for p in range(1, 8):
        out_ref[p] = out_ref[0]


def stats(at, items, users, own):
    return pl.pallas_call(
        stats_kernel,
        in_specs=[SMEM, VMEM, VMEM, VMEM],
        out_shape=jax.ShapeDtypeStruct((8, 24, BLK), F32),
        scratch_shapes=[pltpu.VMEM((ROWS, BLK), F32)] * 2,
        compiler_params=PARAMS,
        name="stats",
    )(at, items, users, own)


def grads_kernel(
    at_ref, items_ref, users_ref, got_ref, gi_ref, keep_ref, give_ref,
    acc_ref, turned_ref, index_ref, even_ref, odd_ref, deven_ref, dodd_ref,
):
    turned_ref[...] = items_ref[...].T
    spot = lax.broadcasted_iota(jnp.int32, (ROWS, BLK), 0)
    index_ref[...] = (spot // BLK) * ROWS + spot % BLK + at_ref[16]
    acc_ref[...] = jnp.zeros_like(acc_ref)

    def chunk(c):
        return users_ref[pl.ds(pl.multiple_of(at_ref[c], BLK), BLK), :]

    def score(c, buffer):
        buffer[...] = dot(items_ref[...], chunk(c), (1, 1))

    def weigh(c, buffer, dbuffer):
        tops = got_ref[:, pl.ds(c, 1), :].reshape(8, BLK)
        parts = got_ref[:, pl.ds(8 + c, 1), :].reshape(8, BLK)
        top = jnp.max(tops, axis=0, keepdims=True)
        total = top + jnp.log(jnp.sum(parts * jnp.exp(tops - top), axis=0, keepdims=True))
        weight = got_ref[c, 16:17, :]
        target = got_ref[c, 17:18, :].astype(jnp.int32)
        chosen = (index_ref[...] == target).astype(F32)
        dbuffer[...] = (weight * (jnp.exp(buffer[...] - total) - chosen)).astype(BF16)

    def multiply(c, dbuffer):
        part = dot(turned_ref[...], dbuffer[...], (1, 0))
        slot = at_ref[8 + c]

        @pl.when(slot < 4)
        def _():
            keep_ref[slot] = part

        @pl.when(slot >= 4)
        def _():
            give_ref[slot - 4] = part

        acc_ref[...] += dot(dbuffer[...], chunk(c), (1, 0))

    score(0, even_ref)
    weigh(0, even_ref, deven_ref)
    score(1, odd_ref)

    def step(i, carry):
        weigh(2 * i + 1, odd_ref, dodd_ref)
        score(2 * i + 2, even_ref)
        multiply(2 * i, deven_ref)
        weigh(2 * i + 2, even_ref, deven_ref)
        score(2 * i + 3, odd_ref)
        multiply(2 * i + 1, dodd_ref)
        return carry

    lax.fori_loop(0, 3, step, 0)
    weigh(7, odd_ref, dodd_ref)
    multiply(6, deven_ref)
    multiply(7, dodd_ref)
    gi_ref[...] = acc_ref[...].astype(BF16)


def grads(at, items, users, got):
    share = jax.ShapeDtypeStruct((4, 256, BLK), F32)
    return pl.pallas_call(
        grads_kernel,
        in_specs=[SMEM, VMEM, VMEM, VMEM],
        out_shape=[jax.ShapeDtypeStruct((ROWS, 256), BF16), share, share],
        scratch_shapes=[
            pltpu.VMEM((ROWS, 256), F32),
            pltpu.VMEM((256, ROWS), BF16),
            pltpu.VMEM((ROWS, BLK), jnp.int32),
            pltpu.VMEM((ROWS, BLK), F32),
            pltpu.VMEM((ROWS, BLK), F32),
            pltpu.VMEM((ROWS, BLK), BF16),
            pltpu.VMEM((ROWS, BLK), BF16),
        ],
        compiler_params=PARAMS,
        name="grads",
    )(at, items, users, got)


def thirds(value):
    high = value.astype(BF16)
    rest = value - high.astype(F32)
    middle = rest.astype(BF16)
    return high, middle, (rest - middle.astype(F32)).astype(BF16)


def pack_kernel(parts_ref, owner_ref, rank_ref, out_ref):
    value = jnp.sum(parts_ref[...].astype(F32), axis=0)
    pieces = thirds(value)
    lane = lax.broadcasted_iota(jnp.int32, (64 * 8, BLK), 0)
    halves = []
    for h in range(2):
        rank = rank_ref[...] - 8 * h
        slot = jnp.where((rank >= 0) & (rank < 8), owner_ref[...] * 8 + rank, -1)
        pick = (lane == slot).astype(F32).astype(BF16)
        halves.append(sum(dot(pick, piece, (1, 0)) for piece in pieces))
    for g in range(4):
        share = slice(64 * g, 64 * g + 64)
        both = jnp.concatenate([halves[0][:, share], halves[1][:, share]], axis=1)
        out_ref[g] = both.reshape(64, 8, 128)


def pack(parts, owner, rank):
    return pl.pallas_call(
        pack_kernel,
        in_specs=[VMEM] * 3,
        out_shape=jax.ShapeDtypeStruct((4, 64, 8, 128), F32),
        compiler_params=PARAMS,
        name="pack",
    )(parts, owner, rank)


def table_kernel(got_ref, ids_ref, out_ref, pick_ref, kept_ref):
    both = got_ref[...].T
    value = jnp.concatenate([both[:64], both[64:]], axis=1)
    pieces = jnp.concatenate(thirds(value), axis=0)
    ids = ids_ref[...]
    upper = ids >> 8
    lower = ids & 255
    pick = (lax.broadcasted_iota(jnp.int32, (256, TABLE), 0) == lower).astype(F32).astype(BF16)
    pick_ref[...] = pick.T

    def step(j, carry):
        for q in range(4):
            keep = jnp.broadcast_to((upper == 4 * j + q).astype(F32), (16, TABLE)).astype(BF16)
            kept_ref[q * 192 : (q + 1) * 192, :] = pieces * jnp.concatenate([keep] * 12, axis=0)
        part = dot(kept_ref[...], pick_ref[...], (1, 0))
        for q in range(4):
            at = pl.multiple_of((4 * j + q) * 256, 256)
            own = part[q * 192 : (q + 1) * 192]
            out_ref[:, pl.ds(at, 256)] = own[:64] + own[64:128] + own[128:]
        return carry

    lax.fori_loop(0, 4, step, 0)


def table(got, ids):
    return pl.pallas_call(
        table_kernel,
        in_specs=[VMEM] * 2,
        out_shape=jax.ShapeDtypeStruct((64, TABLE), F32),
        scratch_shapes=[pltpu.VMEM((TABLE, 256), BF16), pltpu.VMEM((768, TABLE), BF16)],
        compiler_params=PARAMS,
        name="table",
    )(got, ids)


def tower(features, w_first, w_second):
    pre_act = jnp.dot(features, w_first, preferred_element_type=F32)
    hidden = jax.nn.silu(pre_act).astype(BF16)
    return pre_act, hidden, jnp.dot(hidden, w_second, preferred_element_type=F32).astype(BF16)


def step_body(
    user_features, w_first, w_second, item_embed, example_weight, positive, item_owner, item_row
):
    features = user_features[0]
    owner = item_owner.reshape(1, BLK)
    items = to_all(item_embed[0], "z").reshape(ROWS, 256)
    pair = jnp.concatenate([features, shifted(features, "k", 1)], axis=0)
    block = jnp.concatenate([pair] + [shifted(pair, "x", d) for d in range(1, 4)], axis=0)
    _, _, users = tower(block, w_first, w_second)
    chunk = jnp.arange(8, dtype=jnp.int32)
    other = (chunk % 2) ^ lax.axis_index("k")
    back = (lax.axis_index("x") - chunk // 2) & 3
    ahead = (chunk // 2 - lax.axis_index("x")) & 3
    base = (lax.axis_index(XK) * BLK).reshape(1)
    at = jnp.concatenate([(2 * back + other) * BLK, ahead + 4 * other, base]).astype(jnp.int32)

    member = (owner == lax.broadcasted_iota(jnp.int32, (64, 1), 0)).astype(F32)
    order = lax.broadcasted_iota(jnp.int32, (BLK, BLK), 0) < lax.broadcasted_iota(jnp.int32, (BLK, BLK), 1)
    before = dot(member.astype(BF16), order.astype(BF16), (1, 0))
    rank = jnp.sum(before * member, axis=0, keepdims=True).astype(jnp.int32)
    slot = owner * CAP + rank
    held = (slot == lax.broadcasted_iota(jnp.int32, (64 * CAP, 1), 0)).astype(jnp.int32)
    rows = jnp.sum(held * (item_row + 1), axis=1) - 1
    ids = exchange(rows.reshape(64, CAP), ZXK)
    ids = joined(ids, "y")
    ids = jnp.concatenate([ids[:, :8].reshape(1, -1), ids[:, 8:].reshape(1, -1)], axis=1)

    own = jnp.concatenate(
        [example_weight, positive.astype(F32), jnp.zeros((6, BLK), F32)], axis=0
    )
    got = exchange(stats(at[:8], items, users, own), XK)
    gi, keep, give = grads(at, items, users, got)
    gi = exchange(gi.reshape(8, BLK, 256), "z")
    gu = keep + shifted(give, "k", 1)
    grad_user = gu[0]
    for d in range(1, 4):
        grad_user = grad_user + shifted(gu[d], "x", d)
    grad_user = grad_user.T.astype(BF16)

    pre_act, hidden, _ = tower(features, w_first, w_second)
    d_second = dot(hidden, grad_user, (0, 0))
    back_grad = dot(grad_user, w_second, (1, 1))
    gate = jax.nn.sigmoid(pre_act)
    grad_pre = (back_grad * gate * (1.0 + pre_act * (1.0 - gate))).astype(BF16)
    d_first = dot(features, grad_pre, (0, 0))
    both = jnp.concatenate([d_first, d_second], axis=0)
    both = summed_share(both, "k")
    both = summed_share(both, "y")
    both = summed_share(both, "x")
    for step in (1, 2, 4):
        both = both + lax.ppermute(both, "z", [(i, i ^ step) for i in range(8)])

    send = pack(gi, owner, rank).reshape(256, 8, 128)
    came = exchange(send, YZXK).reshape(256 * 8, 128)
    both = to_all(both, KYX).reshape(512, 256)
    grad_table = table(came, ids).T
    return both[:256], both[256:], grad_table


def solution(mesh):
    torus = Mesh(mesh.devices.reshape(8, 4, 2, mesh.shape["grp"]), ("z", "x", "k", "y"))
    rows = ("z", "x", "k")
    placed = (
        P("y", rows, None),
        P(),
        P(),
        P("y", rows, None),
        P("y", rows),
        P("y", rows),
        P("y", rows, None),
        P("y", rows),
    )
    return jax.shard_map(
        step_body, mesh=torus, in_specs=placed, out_specs=(P(), P(), P(rows, "y")), check_vma=False
    )
```

```python
import jax
import jax.numpy as jnp
from jax import lax
from jax.experimental import pallas as pl
from jax.experimental.pallas import tpu as pltpu
from jax.sharding import Mesh
from jax.sharding import PartitionSpec as P

TABLE = 4096
CAP = 16
BLK = 256
ROWS = 8 * BLK
XK = ("x", "k")
KYX = ("k", "y", "x")
YZXK = ("y", "z", "x", "k")
F32 = jnp.float32
BF16 = jnp.bfloat16
VMEM = pl.BlockSpec(memory_space=pltpu.VMEM)
SMEM = pl.BlockSpec(memory_space=pltpu.SMEM)


def dot(left, right, dims):
    return lax.dot_general(left, right, ((dims[0:1], dims[1:2]), ((), ())), preferred_element_type=F32)


def exchange(value, axes):
    return lax.all_to_all(value, axes, 0, 0, tiled=True)


def to_all(value, axes):
    return exchange(jnp.broadcast_to(value[None], (lax.axis_size(axes), *value.shape)), axes)


def shifted(value, axis, step):
    count = lax.axis_size(axis)
    return lax.ppermute(value, axis, [(i, (i + step) % count) for i in range(count)])


def place(axis, step=0):
    return (lax.axis_index(axis).astype(jnp.uint32) + jnp.uint32(step)) & jnp.uint32(lax.axis_size(axis) - 1)


def rows_at(value, start, count):
    zero = jnp.uint32(0)
    return lax.dynamic_slice(value, (start,) + (zero,) * (value.ndim - 1), (count, *value.shape[1:]))


def summed_share(value, axis):
    count = lax.axis_size(axis)
    rows = value.shape[0] // count
    total = rows_at(value, place(axis) * jnp.uint32(rows), rows)
    for d in range(1, count):
        total = total + shifted(rows_at(value, place(axis, d) * jnp.uint32(rows), rows), axis, d)
    return total


def joined(value, axis):
    count = lax.axis_size(axis)
    tiles = [value] + [shifted(value, axis, d) for d in range(1, count)]
    rising = [tiles[-d % count] for d in range(count)]
    rows = value.shape[0]
    start = (jnp.uint32(count) - place(axis)) * jnp.uint32(rows)
    return rows_at(jnp.concatenate(rising + rising, axis=0), start, count * rows)


def stats_kernel(at_ref, items_ref, users_ref, own_ref, out_ref):
    for b in range(8):
        scores = dot(items_ref[...], users_ref[b * BLK : (b + 1) * BLK, :], (1, 1))
        top = jnp.max(scores, axis=0, keepdims=True)
        out_ref[0, pl.ds(at_ref[b], 1), :] = top
        out_ref[0, pl.ds(8 + at_ref[b], 1), :] = jnp.sum(jnp.exp(scores - top), axis=0, keepdims=True)
    out_ref[0, 16:40, :] = own_ref[...]
    for p in range(1, 8):
        out_ref[p] = out_ref[0]


def stats(at, items, users, own):
    return pl.pallas_call(
        stats_kernel,
        in_specs=[SMEM, VMEM, VMEM, VMEM],
        out_shape=jax.ShapeDtypeStruct((8, 40, BLK), F32),
        compiler_params=pltpu.CompilerParams(vmem_limit_bytes=20 * 2**20),
        name="stats",
    )(at, items, users, own)


def grads_kernel(
    at_ref, items_ref, users_ref, got_ref, gi_ref, keep_ref, give_ref,
    all_ref, turned_ref, index_ref, ids_ref,
):
    turned_ref[...] = items_ref[...].T
    spot = lax.broadcasted_iota(jnp.int32, (ROWS, BLK), 0)
    index_ref[...] = (spot // BLK) * ROWS + spot % BLK + at_ref[8]
    for b in range(8):
        c = at_ref[b]
        tops = got_ref[:, pl.ds(c, 1), :].reshape(8, BLK)
        parts = got_ref[:, pl.ds(8 + c, 1), :].reshape(8, BLK)
        own = got_ref[pl.ds(c, 1), 16:18, :].reshape(2, BLK)
        weight = own[0:1]
        target = own[1:2].astype(jnp.int32)
        top = jnp.max(tops, axis=0, keepdims=True)
        total = top + jnp.log(jnp.sum(parts * jnp.exp(tops - top), axis=0, keepdims=True))
        total = total - jnp.log(weight)
        scores = dot(items_ref[...], users_ref[b * BLK : (b + 1) * BLK, :], (1, 1))
        share = jnp.exp(scores - total)
        dscore = jnp.where(index_ref[...] == target, share - weight, share).astype(BF16)
        all_ref[:, b * BLK : (b + 1) * BLK] = dscore
        part = dot(turned_ref[...], dscore, (1, 0))
        if b % 2 == 0:
            keep_ref[b // 2] = part
        else:
            give_ref[b // 2] = part
    gi = dot(all_ref[...], users_ref[...], (1, 0)).astype(BF16)
    for z in range(8):
        gi_ref[z, :BLK, :] = gi[z * BLK : (z + 1) * BLK]
    lane = lax.broadcasted_iota(jnp.int32, (8, 128), 1) // CAP
    ids_ref[...] = jnp.zeros_like(ids_ref)
    for y in range(4):
        row = jnp.zeros((8, 128), F32)
        for p in range(8):
            piece = got_ref[p, 24 + 8 * (y // 2) : 32 + 8 * (y // 2), 128 * (y % 2) : 128 * (y % 2) + 128]
            turn = ((p - at_ref[9]) & 7) * CAP
            row = jnp.where(lane == p, pltpu.roll(piece, turn, 1), row)
        high = jnp.floor(row * (1.0 / 64.0))
        ids_ref[:, y, :128] = high
        ids_ref[:, y, 128:] = row - 64.0 * high
    gi_ref[:, BLK:, :] = ids_ref[...].astype(BF16)


def grads(at, items, users, got):
    share = jax.ShapeDtypeStruct((4, 256, BLK), F32)
    return pl.pallas_call(
        grads_kernel,
        in_specs=[SMEM, VMEM, VMEM, VMEM],
        out_shape=[jax.ShapeDtypeStruct((8, BLK + 8, 256), BF16), share, share],
        scratch_shapes=[
            pltpu.VMEM((ROWS, ROWS), BF16),
            pltpu.VMEM((256, ROWS), BF16),
            pltpu.VMEM((ROWS, BLK), jnp.int32),
            pltpu.VMEM((8, 8, 256), F32),
        ],
        compiler_params=pltpu.CompilerParams(vmem_limit_bytes=40 * 2**20),
        name="grads",
    )(at, items, users, got)


def thirds(value):
    high = value.astype(BF16)
    rest = value - high.astype(F32)
    middle = rest.astype(BF16)
    return high, middle, (rest - middle.astype(F32)).astype(BF16)


def pack_kernel(parts_ref, owner_ref, rank_ref, out_ref):
    value = sum(parts_ref[z, :BLK, :].astype(F32) for z in range(8))
    pieces = thirds(value)
    lane = lax.broadcasted_iota(jnp.int32, (64 * 8, BLK), 0)
    halves = []
    for h in range(2):
        rank = rank_ref[...] - 8 * h
        slot = jnp.where((rank >= 0) & (rank < 8), owner_ref[...] * 8 + rank, -1)
        pick = (lane == slot).astype(F32).astype(BF16)
        halves.append(sum(dot(pick, piece, (1, 0)) for piece in pieces))
    for g in range(4):
        share = slice(64 * g, 64 * g + 64)
        both = jnp.concatenate([halves[0][:, share], halves[1][:, share]], axis=1)
        out_ref[g] = both.reshape(64, 8, 128)


def pack(parts, owner, rank):
    return pl.pallas_call(
        pack_kernel,
        in_specs=[VMEM] * 3,
        out_shape=jax.ShapeDtypeStruct((4, 64, 8, 128), F32),
        compiler_params=pltpu.CompilerParams(vmem_limit_bytes=16 * 2**20),
        name="pack",
    )(parts, owner, rank)


def table_kernel(got_ref, ids_ref, out_ref, pick_ref, kept_ref):
    both = got_ref[...].T
    value = jnp.concatenate([both[:64], both[64:]], axis=1)
    pieces = jnp.concatenate(thirds(value), axis=0)
    ids = ids_ref[...]
    upper = ids >> 8
    lower = ids & 255
    pick = (lax.broadcasted_iota(jnp.int32, (256, TABLE), 0) == lower).astype(F32).astype(BF16)
    pick_ref[...] = pick.T

    def step(j, carry):
        for q in range(4):
            keep = jnp.broadcast_to((upper == 4 * j + q).astype(F32), (16, TABLE)).astype(BF16)
            kept_ref[q * 192 : (q + 1) * 192, :] = pieces * jnp.concatenate([keep] * 12, axis=0)
        part = dot(kept_ref[...], pick_ref[...], (1, 0))
        for q in range(4):
            at = pl.multiple_of((4 * j + q) * 256, 256)
            own = part[q * 192 : (q + 1) * 192]
            out_ref[:, pl.ds(at, 256)] = own[:64] + own[64:128] + own[128:]
        return carry

    lax.fori_loop(0, 4, step, 0)


def table(got, ids):
    return pl.pallas_call(
        table_kernel,
        in_specs=[VMEM] * 2,
        out_shape=jax.ShapeDtypeStruct((64, TABLE), F32),
        scratch_shapes=[pltpu.VMEM((TABLE, 256), BF16), pltpu.VMEM((768, TABLE), BF16)],
        compiler_params=pltpu.CompilerParams(vmem_limit_bytes=36 * 2**20),
        name="table",
    )(got, ids)


def tower(features, w_first, w_second):
    pre_act = jnp.dot(features, w_first, preferred_element_type=F32)
    hidden = jax.nn.silu(pre_act).astype(BF16)
    return pre_act, hidden, jnp.dot(hidden, w_second, preferred_element_type=F32).astype(BF16)


def step_body(
    user_features, w_first, w_second, item_embed, example_weight, positive, item_owner, item_row
):
    features = user_features[0]
    owner = item_owner.reshape(1, BLK)
    items = to_all(item_embed[0], "z").reshape(ROWS, 256)
    pair = jnp.concatenate([features, shifted(features, "k", 1)], axis=0)
    block = jnp.concatenate([pair] + [shifted(pair, "x", d) for d in range(1, 4)], axis=0)
    _, _, users = tower(block, w_first, w_second)
    block_no = jnp.arange(8, dtype=jnp.int32)
    source = 2 * ((lax.axis_index("x") - block_no // 2) & 3) + ((block_no % 2) ^ lax.axis_index("k"))
    own_place = lax.axis_index(XK).reshape(1)
    at = jnp.concatenate([source, own_place * BLK, own_place]).astype(jnp.int32)

    member = (owner == lax.broadcasted_iota(jnp.int32, (64, 1), 0)).astype(F32)
    order = lax.broadcasted_iota(jnp.int32, (BLK, BLK), 0) < lax.broadcasted_iota(jnp.int32, (BLK, BLK), 1)
    before = dot(member.astype(BF16), order.astype(BF16), (1, 0))
    rank = jnp.sum(before * member, axis=0, keepdims=True).astype(jnp.int32)
    slot = owner * CAP + rank
    held = (slot == lax.broadcasted_iota(jnp.int32, (64 * CAP, 1), 0)).astype(jnp.int32)
    rows = jnp.sum(held * (item_row + 1), axis=1).astype(F32).reshape(64, CAP)
    rows = joined(rows, "y")
    rows = rows.reshape(2, 2, 8, 128).swapaxes(1, 2).reshape(16, BLK)
    own = jnp.concatenate(
        [example_weight, positive.astype(F32), jnp.zeros((6, BLK), F32), rows], axis=0
    )
    got = exchange(stats(at, items, users, own), XK)
    gi, keep, give = grads(at, items, users, got)
    gi = exchange(gi, "z")
    gu = keep + shifted(give, "k", 1)
    grad_user = gu[0]
    for d in range(1, 4):
        grad_user = grad_user + shifted(gu[d], "x", -d)
    grad_user = grad_user.T.astype(BF16)
    ids = gi[:, BLK : BLK + 4, :].astype(F32)
    ids = (64.0 * ids[:, :, :128] + ids[:, :, 128:]).astype(jnp.int32) - 1
    ids = ids.swapaxes(0, 1).reshape(4 * 64, CAP)
    ids = jnp.concatenate([ids[:, :8].reshape(1, -1), ids[:, 8:].reshape(1, -1)], axis=1)

    pre_act, hidden, _ = tower(features, w_first, w_second)
    d_second = dot(hidden, grad_user, (0, 0))
    back_grad = dot(grad_user, w_second, (1, 1))
    gate = jax.nn.sigmoid(pre_act)
    grad_pre = (back_grad * gate * (1.0 + pre_act * (1.0 - gate))).astype(BF16)
    d_first = dot(features, grad_pre, (0, 0))
    both = jnp.concatenate([d_first, d_second], axis=0)
    both = summed_share(both, "k")
    both = summed_share(both, "y")
    both = summed_share(both, "x")
    for step in (1, 2, 4):
        both = both + lax.ppermute(both, "z", [(i, i ^ step) for i in range(8)])

    send = pack(gi, owner, rank).reshape(256, 8, 128)
    came = exchange(send, YZXK).reshape(256 * 8, 128)
    both = to_all(both, KYX).reshape(512, 256)
    grad_table = table(came, ids).T
    return both[:256], both[256:], grad_table


def solution(mesh):
    torus = Mesh(mesh.devices.reshape(8, 4, 2, mesh.shape["grp"]), ("z", "x", "k", "y"))
    rows = ("z", "x", "k")
    placed = (
        P("y", rows, None),
        P(),
        P(),
        P("y", rows, None),
        P("y", rows),
        P("y", rows),
        P("y", rows, None),
        P("y", rows),
    )
    return jax.shard_map(step_body, mesh=torus, in_specs=placed, out_specs=(P(), P(), P(rows, "y")), check_vma=False)
```

```python
import jax
import jax.numpy as jnp
from jax import lax
from jax.experimental import pallas as pl
from jax.experimental.pallas import tpu as pltpu
from jax.sharding import Mesh
from jax.sharding import PartitionSpec as P

TABLE = 4096
CAP = 16
BLK = 256
ROWS = 8 * BLK
XK = ("x", "k")
KYX = ("k", "y", "x")
YZXK = ("y", "z", "x", "k")
F32 = jnp.float32
BF16 = jnp.bfloat16
VMEM = pl.BlockSpec(memory_space=pltpu.VMEM)
SMEM = pl.BlockSpec(memory_space=pltpu.SMEM)


def dot(left, right, dims):
    return lax.dot_general(left, right, ((dims[0:1], dims[1:2]), ((), ())), preferred_element_type=F32)


def exchange(value, axes):
    return lax.all_to_all(value, axes, 0, 0, tiled=True)


def to_all(value, axes):
    return exchange(jnp.broadcast_to(value[None], (lax.axis_size(axes), *value.shape)), axes)


def shifted(value, axis, step):
    count = lax.axis_size(axis)
    return lax.ppermute(value, axis, [(i, (i + step) % count) for i in range(count)])


def place(axis, step=0):
    return (lax.axis_index(axis).astype(jnp.uint32) + jnp.uint32(step)) & jnp.uint32(lax.axis_size(axis) - 1)


def rows_at(value, start, count):
    zero = jnp.uint32(0)
    return lax.dynamic_slice(value, (start,) + (zero,) * (value.ndim - 1), (count, *value.shape[1:]))


def summed_share(value, axis):
    count = lax.axis_size(axis)
    rows = value.shape[0] // count
    total = rows_at(value, place(axis) * jnp.uint32(rows), rows)
    for d in range(1, count):
        total = total + shifted(rows_at(value, place(axis, d) * jnp.uint32(rows), rows), axis, d)
    return total


def joined(value, axis):
    count = lax.axis_size(axis)
    tiles = [value] + [shifted(value, axis, d) for d in range(1, count)]
    rising = [tiles[-d % count] for d in range(count)]
    rows = value.shape[0]
    start = (jnp.uint32(count) - place(axis)) * jnp.uint32(rows)
    return rows_at(jnp.concatenate(rising + rising, axis=0), start, count * rows)


def stats_kernel(at_ref, items_ref, users_ref, own_ref, out_ref):
    for b in range(8):
        scores = dot(items_ref[...], users_ref[b * BLK : (b + 1) * BLK, :], (1, 1))
        top = jnp.max(scores, axis=0, keepdims=True)
        out_ref[0, pl.ds(at_ref[b], 1), :] = top
        out_ref[0, pl.ds(8 + at_ref[b], 1), :] = jnp.sum(jnp.exp(scores - top), axis=0, keepdims=True)
    out_ref[0, 16:40, :] = own_ref[...]
    for p in range(1, 8):
        out_ref[p] = out_ref[0]


def stats(at, items, users, own):
    return pl.pallas_call(
        stats_kernel,
        in_specs=[SMEM, VMEM, VMEM, VMEM],
        out_shape=jax.ShapeDtypeStruct((8, 40, BLK), F32),
        compiler_params=pltpu.CompilerParams(vmem_limit_bytes=20 * 2**20),
        name="stats",
    )(at, items, users, own)


def grads_kernel(
    at_ref, items_ref, users_ref, got_ref, gi_ref, keep_ref, give_ref,
    all_ref, turned_ref, index_ref, ids_ref,
):
    turned_ref[...] = items_ref[...].T
    spot = lax.broadcasted_iota(jnp.int32, (ROWS, BLK), 0)
    index_ref[...] = (spot // BLK) * ROWS + spot % BLK + at_ref[8]
    for b in range(8):
        c = at_ref[b]
        tops = got_ref[:, pl.ds(c, 1), :].reshape(8, BLK)
        parts = got_ref[:, pl.ds(8 + c, 1), :].reshape(8, BLK)
        own = got_ref[pl.ds(c, 1), 16:18, :].reshape(2, BLK)
        weight = own[0:1]
        target = own[1:2].astype(jnp.int32)
        top = jnp.max(tops, axis=0, keepdims=True)
        total = top + jnp.log(jnp.sum(parts * jnp.exp(tops - top), axis=0, keepdims=True))
        total = total - jnp.log(weight)
        scores = dot(items_ref[...], users_ref[b * BLK : (b + 1) * BLK, :], (1, 1))
        share = jnp.exp(scores - total)
        dscore = jnp.where(index_ref[...] == target, share - weight, share).astype(BF16)
        all_ref[:, b * BLK : (b + 1) * BLK] = dscore
        part = dot(turned_ref[...], dscore, (1, 0))
        if b % 2 == 0:
            keep_ref[b // 2] = part
        else:
            give_ref[b // 2] = part
    largest = jnp.max(jnp.abs(users_ref[...].astype(F32)), axis=0, keepdims=True)
    largest = jnp.maximum(jnp.max(largest, axis=1, keepdims=True) * 416.0, 1e-30)
    power = jnp.ceil(jnp.log(largest) * 1.4426950408889634)
    gi = dot(all_ref[...], users_ref[...], (1, 0)) * jnp.exp2(15.0 - power)
    for z in range(8):
        gi_ref[z, :BLK, :] = gi[z * BLK : (z + 1) * BLK]
    lane = lax.broadcasted_iota(jnp.int32, (8, 128), 1) // CAP
    ids_ref[...] = jnp.zeros_like(ids_ref)
    for y in range(4):
        row = jnp.zeros((8, 128), F32)
        for p in range(8):
            piece = got_ref[p, 24 + 8 * (y // 2) : 32 + 8 * (y // 2), 128 * (y % 2) : 128 * (y % 2) + 128]
            turn = ((p - at_ref[9]) & 7) * CAP
            row = jnp.where(lane == p, pltpu.roll(piece, turn, 1), row)
        high = jnp.floor(row * (1.0 / 64.0))
        ids_ref[:, y, :128] = high
        ids_ref[:, y, 128:] = row - 64.0 * high
    ids_ref[:, 4, :] = jnp.broadcast_to(power, (8, 256))
    gi_ref[:, BLK:, :] = ids_ref[...]


def grads(at, items, users, got):
    share = jax.ShapeDtypeStruct((4, 256, BLK), F32)
    return pl.pallas_call(
        grads_kernel,
        in_specs=[SMEM, VMEM, VMEM, VMEM],
        out_shape=[jax.ShapeDtypeStruct((8, BLK + 8, 256), F32), share, share],
        scratch_shapes=[
            pltpu.VMEM((ROWS, ROWS), BF16),
            pltpu.VMEM((256, ROWS), BF16),
            pltpu.VMEM((ROWS, BLK), jnp.int32),
            pltpu.VMEM((8, 8, 256), F32),
        ],
        compiler_params=pltpu.CompilerParams(vmem_limit_bytes=40 * 2**20),
        name="grads",
    )(at, items, users, got)


def pack_kernel(item_ref, owner_ref, rank_ref, out_ref):
    lane = lax.broadcasted_iota(jnp.int32, (64 * 8, BLK), 0)
    halves = []
    for h in range(2):
        rank = rank_ref[...] - 8 * h
        slot = jnp.where((rank >= 0) & (rank < 8), owner_ref[...] * 8 + rank, -1)
        pick = (lane == slot).astype(F32).astype(BF16)
        halves.append(dot(pick, item_ref[...], (1, 0)))
    for g in range(4):
        share = slice(64 * g, 64 * g + 64)
        both = jnp.concatenate([halves[0][:, share], halves[1][:, share]], axis=1)
        out_ref[g * 512 : (g + 1) * 512, :] = both.astype(BF16)


def pack(item, owner, rank):
    return pl.pallas_call(
        pack_kernel,
        in_specs=[VMEM] * 3,
        out_shape=jax.ShapeDtypeStruct((4 * 512, 128), BF16),
        compiler_params=pltpu.CompilerParams(vmem_limit_bytes=16 * 2**20),
        name="pack",
    )(item, owner, rank)


def table_kernel(got_ref, ids_ref, out_ref, pick_ref, kept_ref):
    both = got_ref[...].T
    value = jnp.concatenate([both[:64], both[64:]], axis=1)
    ids = ids_ref[...]
    upper = ids >> 8
    lower = ids & 255
    pick = (lax.broadcasted_iota(jnp.int32, (256, TABLE), 0) == lower).astype(F32).astype(BF16)
    pick_ref[...] = pick.T

    def step(j, carry):
        for q in range(4):
            keep = jnp.broadcast_to((upper == 4 * j + q).astype(F32), (16, TABLE)).astype(BF16)
            kept_ref[q * 64 : (q + 1) * 64, :] = value * jnp.concatenate([keep] * 4, axis=0)
        part = dot(kept_ref[...], pick_ref[...], (1, 0))
        for q in range(4):
            at = pl.multiple_of((4 * j + q) * 256, 256)
            out_ref[:, pl.ds(at, 256)] = part[q * 64 : (q + 1) * 64]
        return carry

    lax.fori_loop(0, 4, step, 0)


def table(got, ids):
    return pl.pallas_call(
        table_kernel,
        in_specs=[VMEM] * 2,
        out_shape=jax.ShapeDtypeStruct((64, TABLE), F32),
        scratch_shapes=[pltpu.VMEM((TABLE, 256), BF16), pltpu.VMEM((256, TABLE), BF16)],
        compiler_params=pltpu.CompilerParams(vmem_limit_bytes=28 * 2**20),
        name="table",
    )(got, ids)


def tower(features, w_first, w_second):
    pre_act = jnp.dot(features, w_first, preferred_element_type=F32)
    hidden = jax.nn.silu(pre_act).astype(BF16)
    return pre_act, hidden, jnp.dot(hidden, w_second, preferred_element_type=F32).astype(BF16)


def step_body(
    user_features, w_first, w_second, item_embed, example_weight, positive, item_owner, item_row
):
    features = user_features[0]
    owner = item_owner.reshape(1, BLK)
    items = to_all(item_embed[0], "z").reshape(ROWS, 256)
    pair = jnp.concatenate([features, shifted(features, "k", 1)], axis=0)
    block = jnp.concatenate([pair] + [shifted(pair, "x", d) for d in range(1, 4)], axis=0)
    _, _, users = tower(block, w_first, w_second)
    block_no = jnp.arange(8, dtype=jnp.int32)
    source = 2 * ((lax.axis_index("x") - block_no // 2) & 3) + ((block_no % 2) ^ lax.axis_index("k"))
    own_place = lax.axis_index(XK).reshape(1)
    at = jnp.concatenate([source, own_place * BLK, own_place]).astype(jnp.int32)

    member = (owner == lax.broadcasted_iota(jnp.int32, (64, 1), 0)).astype(F32)
    order = lax.broadcasted_iota(jnp.int32, (BLK, BLK), 0) < lax.broadcasted_iota(jnp.int32, (BLK, BLK), 1)
    before = dot(member.astype(BF16), order.astype(BF16), (1, 0))
    rank = jnp.sum(before * member, axis=0, keepdims=True).astype(jnp.int32)
    slot = owner * CAP + rank
    held = (slot == lax.broadcasted_iota(jnp.int32, (64 * CAP, 1), 0)).astype(jnp.int32)
    rows = jnp.sum(held * (item_row + 1), axis=1).astype(F32).reshape(64, CAP)
    rows = joined(rows, "y")
    rows = rows.reshape(2, 2, 8, 128).swapaxes(1, 2).reshape(16, BLK)
    own = jnp.concatenate(
        [example_weight, positive.astype(F32), jnp.zeros((6, BLK), F32), rows], axis=0
    )
    got = exchange(stats(at, items, users, own), XK)
    gi, keep, give = grads(at, items, users, got)
    gi = exchange(gi.astype(jnp.float16), "z")
    scale = jnp.exp2(gi[:, BLK + 4, 0].astype(F32) - 15.0)
    item = sum(gi[z, :BLK].astype(F32) * scale[z] for z in range(8)).astype(BF16)
    gu = keep + shifted(give, "k", 1)
    grad_user = gu[0]
    for d in range(1, 4):
        grad_user = grad_user + shifted(gu[d], "x", -d)
    grad_user = grad_user.T.astype(BF16)
    ids = gi[:, BLK : BLK + 4, :].astype(F32)
    ids = (64.0 * ids[:, :, :128] + ids[:, :, 128:]).astype(jnp.int32) - 1
    ids = ids.swapaxes(0, 1).reshape(4 * 64, CAP)
    ids = jnp.concatenate([ids[:, :8].reshape(1, -1), ids[:, 8:].reshape(1, -1)], axis=1)

    pre_act, hidden, _ = tower(features, w_first, w_second)
    d_second = dot(hidden, grad_user, (0, 0))
    back_grad = dot(grad_user, w_second, (1, 1))
    gate = jax.nn.sigmoid(pre_act)
    grad_pre = (back_grad * gate * (1.0 + pre_act * (1.0 - gate))).astype(BF16)
    d_first = dot(features, grad_pre, (0, 0))
    both = jnp.concatenate([d_first, d_second], axis=0)
    both = summed_share(both, "k")
    both = summed_share(both, "y")
    both = summed_share(both, "x")
    for step in (1, 2, 4):
        both = both + lax.ppermute(both, "z", [(i, i ^ step) for i in range(8)])

    send = pack(item, owner, rank).reshape(256, 8, 128)
    came = exchange(send, YZXK).reshape(256 * 8, 128)
    both = to_all(both, KYX).reshape(512, 256)
    grad_table = table(came, ids).T
    return both[:256], both[256:], grad_table


def solution(mesh):
    torus = Mesh(mesh.devices.reshape(8, 4, 2, mesh.shape["grp"]), ("z", "x", "k", "y"))
    rows = ("z", "x", "k")
    placed = (
        P("y", rows, None),
        P(),
        P(),
        P("y", rows, None),
        P("y", rows),
        P("y", rows),
        P("y", rows, None),
        P("y", rows),
    )
    return jax.shard_map(step_body, mesh=torus, in_specs=placed, out_specs=(P(), P(), P(rows, "y")), check_vma=False)
```

```python
import jax
import jax.numpy as jnp
from jax import lax
from jax.experimental import pallas as pl
from jax.experimental.pallas import tpu as pltpu
from jax.sharding import Mesh
from jax.sharding import PartitionSpec as P

TABLE = 4096
CAP = 16
BLK = 256
ROWS = 8 * BLK
XK = ("x", "k")
KYX = ("k", "y", "x")
YZXK = ("y", "z", "x", "k")
F32 = jnp.float32
BF16 = jnp.bfloat16
VMEM = pl.BlockSpec(memory_space=pltpu.VMEM)
SMEM = pl.BlockSpec(memory_space=pltpu.SMEM)


def dot(left, right, dims):
    return lax.dot_general(left, right, ((dims[0:1], dims[1:2]), ((), ())), preferred_element_type=F32)


def exchange(value, axes):
    return lax.all_to_all(value, axes, 0, 0, tiled=True)


def to_all(value, axes):
    return exchange(jnp.broadcast_to(value[None], (lax.axis_size(axes), *value.shape)), axes)


def shifted(value, axis, step):
    count = lax.axis_size(axis)
    return lax.ppermute(value, axis, [(i, (i + step) % count) for i in range(count)])


def place(axis, step=0):
    return (lax.axis_index(axis).astype(jnp.uint32) + jnp.uint32(step)) & jnp.uint32(lax.axis_size(axis) - 1)


def rows_at(value, start, count):
    zero = jnp.uint32(0)
    return lax.dynamic_slice(value, (start,) + (zero,) * (value.ndim - 1), (count, *value.shape[1:]))


def summed_share(value, axis):
    count = lax.axis_size(axis)
    rows = value.shape[0] // count
    total = rows_at(value, place(axis) * jnp.uint32(rows), rows)
    for d in range(1, count):
        total = total + shifted(rows_at(value, place(axis, d) * jnp.uint32(rows), rows), axis, d)
    return total


def joined(value, axis):
    count = lax.axis_size(axis)
    tiles = [value] + [shifted(value, axis, d) for d in range(1, count)]
    rising = [tiles[-d % count] for d in range(count)]
    rows = value.shape[0]
    start = (jnp.uint32(count) - place(axis)) * jnp.uint32(rows)
    return rows_at(jnp.concatenate(rising + rising, axis=0), start, count * rows)


def stats_kernel(at_ref, items_ref, users_ref, own_ref, out_ref):
    for b in range(8):
        scores = dot(items_ref[...], users_ref[b * BLK : (b + 1) * BLK, :], (1, 1))
        top = jnp.max(scores, axis=0, keepdims=True)
        out_ref[0, pl.ds(at_ref[b], 1), :] = top
        out_ref[0, pl.ds(8 + at_ref[b], 1), :] = jnp.sum(jnp.exp(scores - top), axis=0, keepdims=True)
    out_ref[0, 16:40, :] = own_ref[...]
    for p in range(1, 8):
        out_ref[p] = out_ref[0]


def stats(at, items, users, own):
    return pl.pallas_call(
        stats_kernel,
        in_specs=[SMEM, VMEM, VMEM, VMEM],
        out_shape=jax.ShapeDtypeStruct((8, 40, BLK), F32),
        compiler_params=pltpu.CompilerParams(vmem_limit_bytes=20 * 2**20),
        name="stats",
    )(at, items, users, own)


def users_kernel(
    at_ref, items_ref, users_ref, got_ref, all_ref, keep_ref, give_ref, turned_ref, index_ref
):
    turned_ref[...] = items_ref[...].T
    spot = lax.broadcasted_iota(jnp.int32, (ROWS, BLK), 0)
    index_ref[...] = (spot // BLK) * ROWS + spot % BLK + at_ref[8]
    for b in range(8):
        c = at_ref[b]
        tops = got_ref[:, pl.ds(c, 1), :].reshape(8, BLK)
        parts = got_ref[:, pl.ds(8 + c, 1), :].reshape(8, BLK)
        own = got_ref[pl.ds(c, 1), 16:18, :].reshape(2, BLK)
        weight = own[0:1]
        target = own[1:2].astype(jnp.int32)
        top = jnp.max(tops, axis=0, keepdims=True)
        total = top + jnp.log(jnp.sum(parts * jnp.exp(tops - top), axis=0, keepdims=True))
        total = total - jnp.log(weight)
        scores = dot(items_ref[...], users_ref[b * BLK : (b + 1) * BLK, :], (1, 1))
        share = jnp.exp(scores - total)
        dscore = jnp.where(index_ref[...] == target, share - weight, share).astype(BF16)
        all_ref[:, b * BLK : (b + 1) * BLK] = dscore
        part = dot(turned_ref[...], dscore, (1, 0))
        if b % 2 == 0:
            keep_ref[b // 2] = part
        else:
            give_ref[b // 2] = part


def user_side(at, items, users, got):
    share = jax.ShapeDtypeStruct((4, 256, BLK), F32)
    return pl.pallas_call(
        users_kernel,
        in_specs=[SMEM, VMEM, VMEM, VMEM],
        out_specs=[VMEM] * 3,
        out_shape=[jax.ShapeDtypeStruct((ROWS, ROWS), BF16), share, share],
        scratch_shapes=[pltpu.VMEM((256, ROWS), BF16), pltpu.VMEM((ROWS, BLK), jnp.int32)],
        compiler_params=pltpu.CompilerParams(vmem_limit_bytes=32 * 2**20),
        name="user_side",
    )(at, items, users, got)


def items_kernel(at_ref, all_ref, users_ref, got_ref, gi_ref, ids_ref):
    largest = jnp.max(jnp.abs(users_ref[...].astype(F32)), axis=0, keepdims=True)
    largest = jnp.maximum(jnp.max(largest, axis=1, keepdims=True) * 416.0, 1e-30)
    power = jnp.ceil(jnp.log(largest) * 1.4426950408889634)
    gi = dot(all_ref[...], users_ref[...], (1, 0)) * jnp.exp2(15.0 - power)
    for z in range(8):
        gi_ref[z, :BLK, :] = gi[z * BLK : (z + 1) * BLK]
    lane = lax.broadcasted_iota(jnp.int32, (8, 128), 1) // CAP
    ids_ref[...] = jnp.zeros_like(ids_ref)
    for y in range(4):
        row = jnp.zeros((8, 128), F32)
        for p in range(8):
            piece = got_ref[p, 24 + 8 * (y // 2) : 32 + 8 * (y // 2), 128 * (y % 2) : 128 * (y % 2) + 128]
            turn = ((p - at_ref[9]) & 7) * CAP
            row = jnp.where(lane == p, pltpu.roll(piece, turn, 1), row)
        high = jnp.floor(row * (1.0 / 64.0))
        ids_ref[:, y, :128] = high
        ids_ref[:, y, 128:] = row - 64.0 * high
    ids_ref[:, 4, :] = jnp.broadcast_to(power, (8, 256))
    gi_ref[:, BLK:, :] = ids_ref[...]


def item_side(at, dscore, users, got):
    return pl.pallas_call(
        items_kernel,
        in_specs=[SMEM, VMEM, VMEM, VMEM],
        out_specs=VMEM,
        out_shape=jax.ShapeDtypeStruct((8, BLK + 8, 256), F32),
        scratch_shapes=[pltpu.VMEM((8, 8, 256), F32)],
        compiler_params=pltpu.CompilerParams(vmem_limit_bytes=22 * 2**20),
        name="item_side",
    )(at, dscore, users, got)


def tower_kernel(
    core_ref, own_ref, one_ref, two_ref, three_ref, features_ref, first_ref, second_ref,
    keep_ref, give_ref,
):
    grad_user = (own_ref[0] + one_ref[...] + two_ref[...] + three_ref[...]).astype(BF16)
    features = features_ref[...].T
    pre_act = dot(first_ref[...].T, features, (1, 0))
    hidden = jax.nn.silu(pre_act).astype(BF16)
    d_second = dot(hidden, grad_user, (1, 1))
    back_grad = dot(second_ref[...], grad_user, (1, 0))
    gate = jax.nn.sigmoid(pre_act)
    grad_pre = (back_grad * gate * (1.0 + pre_act * (1.0 - gate))).astype(BF16)
    d_first = dot(features, grad_pre, (1, 1))

    @pl.when(core_ref[0] == 0)
    def _():
        keep_ref[...] = d_first
        give_ref[...] = d_second

    @pl.when(core_ref[0] != 0)
    def _():
        keep_ref[...] = d_second
        give_ref[...] = d_first


def tower_grads(core, parts, features, w_first, w_second):
    return pl.pallas_call(
        tower_kernel,
        in_specs=[SMEM] + [VMEM] * 7,
        out_specs=[VMEM] * 2,
        out_shape=[jax.ShapeDtypeStruct((256, 256), F32)] * 2,
        compiler_params=pltpu.CompilerParams(vmem_limit_bytes=16 * 2**20),
        name="tower_grads",
    )(core, *parts, features, w_first, w_second)


def pack_kernel(item_ref, owner_ref, rank_ref, out_ref):
    lane = lax.broadcasted_iota(jnp.int32, (64 * 8, BLK), 0)
    halves = []
    for h in range(2):
        rank = rank_ref[...] - 8 * h
        slot = jnp.where((rank >= 0) & (rank < 8), owner_ref[...] * 8 + rank, -1)
        pick = (lane == slot).astype(F32).astype(BF16)
        halves.append(dot(pick, item_ref[...], (1, 0)))
    for g in range(4):
        share = slice(64 * g, 64 * g + 64)
        both = jnp.concatenate([halves[0][:, share], halves[1][:, share]], axis=1)
        out_ref[g * 512 : (g + 1) * 512, :] = both.astype(BF16)


def pack(item, owner, rank):
    return pl.pallas_call(
        pack_kernel,
        in_specs=[VMEM] * 3,
        out_shape=jax.ShapeDtypeStruct((4 * 512, 128), BF16),
        compiler_params=pltpu.CompilerParams(vmem_limit_bytes=16 * 2**20),
        name="pack",
    )(item, owner, rank)


def table_kernel(got_ref, ids_ref, out_ref, pick_ref, kept_ref):
    both = got_ref[...].T
    value = jnp.concatenate([both[:64], both[64:]], axis=1)
    ids = ids_ref[...]
    upper = ids >> 8
    lower = ids & 255
    pick = (lax.broadcasted_iota(jnp.int32, (256, TABLE), 0) == lower).astype(F32).astype(BF16)
    pick_ref[...] = pick.T

    def step(j, carry):
        for q in range(4):
            keep = jnp.broadcast_to((upper == 4 * j + q).astype(F32), (16, TABLE)).astype(BF16)
            kept_ref[q * 64 : (q + 1) * 64, :] = value * jnp.concatenate([keep] * 4, axis=0)
        part = dot(kept_ref[...], pick_ref[...], (1, 0))
        for q in range(4):
            at = pl.multiple_of((4 * j + q) * 256, 256)
            out_ref[:, pl.ds(at, 256)] = part[q * 64 : (q + 1) * 64]
        return carry

    lax.fori_loop(0, 4, step, 0)


def table(got, ids):
    return pl.pallas_call(
        table_kernel,
        in_specs=[VMEM] * 2,
        out_shape=jax.ShapeDtypeStruct((64, TABLE), F32),
        scratch_shapes=[pltpu.VMEM((TABLE, 256), BF16), pltpu.VMEM((256, TABLE), BF16)],
        compiler_params=pltpu.CompilerParams(vmem_limit_bytes=28 * 2**20),
        name="table",
    )(got, ids)


def tower(features, w_first, w_second):
    pre_act = jnp.dot(features, w_first, preferred_element_type=F32)
    hidden = jax.nn.silu(pre_act).astype(BF16)
    return pre_act, hidden, jnp.dot(hidden, w_second, preferred_element_type=F32).astype(BF16)


def step_body(
    user_features, w_first, w_second, item_embed, example_weight, positive, item_owner, item_row
):
    features = user_features[0]
    owner = item_owner.reshape(1, BLK)
    items = to_all(item_embed[0], "z").reshape(ROWS, 256)
    pair = jnp.concatenate([features, shifted(features, "k", 1)], axis=0)
    block = jnp.concatenate([pair] + [shifted(pair, "x", d) for d in range(1, 4)], axis=0)
    _, _, users = tower(block, w_first, w_second)
    block_no = jnp.arange(8, dtype=jnp.int32)
    source = 2 * ((lax.axis_index("x") - block_no // 2) & 3) + ((block_no % 2) ^ lax.axis_index("k"))
    own_place = lax.axis_index(XK).reshape(1)
    at = jnp.concatenate([source, own_place * BLK, own_place]).astype(jnp.int32)

    member = (owner == lax.broadcasted_iota(jnp.int32, (64, 1), 0)).astype(F32)
    order = lax.broadcasted_iota(jnp.int32, (BLK, BLK), 0) < lax.broadcasted_iota(jnp.int32, (BLK, BLK), 1)
    before = dot(member.astype(BF16), order.astype(BF16), (1, 0))
    rank = jnp.sum(before * member, axis=0, keepdims=True).astype(jnp.int32)
    slot = owner * CAP + rank
    held = (slot == lax.broadcasted_iota(jnp.int32, (64 * CAP, 1), 0)).astype(jnp.int32)
    rows = jnp.sum(held * (item_row + 1), axis=1).astype(F32).reshape(64, CAP)
    rows = joined(rows, "y")
    rows = rows.reshape(2, 2, 8, 128).swapaxes(1, 2).reshape(16, BLK)
    own = jnp.concatenate(
        [example_weight, positive.astype(F32), jnp.zeros((6, BLK), F32), rows], axis=0
    )
    got = exchange(stats(at, items, users, own), XK)
    dscore, keep, give = user_side(at, items, users, got)
    swapped = shifted(give, "k", 1)
    gi = item_side(at, dscore, users, got)
    gi = exchange(gi.astype(jnp.float16), "z")
    gu = keep + swapped
    parts = [gu] + [shifted(gu[d], "x", -d) for d in range(1, 4)]
    scale = jnp.exp2(gi[:, BLK + 4, 0].astype(F32) - 15.0)
    item = sum(gi[z, :BLK].astype(F32) * scale[z] for z in range(8)).astype(BF16)
    ids = gi[:, BLK : BLK + 4, :].astype(F32)
    ids = (64.0 * ids[:, :, :128] + ids[:, :, 128:]).astype(jnp.int32) - 1
    ids = ids.swapaxes(0, 1).reshape(4 * 64, CAP)
    ids = jnp.concatenate([ids[:, :8].reshape(1, -1), ids[:, 8:].reshape(1, -1)], axis=1)

    core = lax.axis_index("k").astype(jnp.int32).reshape(1)
    both, other = tower_grads(core, parts, features, w_first, w_second)
    both = both + shifted(other, "k", 1)
    both = summed_share(both, "y")
    both = summed_share(both, "x")
    for step in (1, 2, 4):
        both = both + lax.ppermute(both, "z", [(i, i ^ step) for i in range(8)])

    send = pack(item, owner, rank).reshape(256, 8, 128)
    came = exchange(send, YZXK).reshape(256 * 8, 128)
    both = to_all(both, KYX).reshape(512, 256)
    grad_table = table(came, ids).T
    return both[:256], both[256:], grad_table


def solution(mesh):
    torus = Mesh(mesh.devices.reshape(8, 4, 2, mesh.shape["grp"]), ("z", "x", "k", "y"))
    rows = ("z", "x", "k")
    placed = (
        P("y", rows, None),
        P(),
        P(),
        P("y", rows, None),
        P("y", rows),
        P("y", rows),
        P("y", rows, None),
        P("y", rows),
    )
    return jax.shard_map(step_body, mesh=torus, in_specs=placed, out_specs=(P(), P(), P(rows, "y")), check_vma=False)
```

```python
import jax
import jax.numpy as jnp
from jax import lax
from jax.experimental import pallas as pl
from jax.experimental.pallas import tpu as pltpu
from jax.sharding import Mesh
from jax.sharding import PartitionSpec as P

TABLE = 4096
CAP = 16
BLK = 256
ROWS = 8 * BLK
XK = ("x", "k")
KYX = ("k", "y", "x")
YZXK = ("y", "z", "x", "k")
F32 = jnp.float32
BF16 = jnp.bfloat16
VMEM = pl.BlockSpec(memory_space=pltpu.VMEM)
SMEM = pl.BlockSpec(memory_space=pltpu.SMEM)


def dot(left, right, dims):
    return lax.dot_general(left, right, ((dims[0:1], dims[1:2]), ((), ())), preferred_element_type=F32)


def exchange(value, axes):
    return lax.all_to_all(value, axes, 0, 0, tiled=True)


def to_all(value, axes):
    return exchange(jnp.broadcast_to(value[None], (lax.axis_size(axes), *value.shape)), axes)


def shifted(value, axis, step):
    count = lax.axis_size(axis)
    return lax.ppermute(value, axis, [(i, (i + step) % count) for i in range(count)])


def place(axis, step=0):
    return (lax.axis_index(axis).astype(jnp.uint32) + jnp.uint32(step)) & jnp.uint32(lax.axis_size(axis) - 1)


def rows_at(value, start, count):
    zero = jnp.uint32(0)
    return lax.dynamic_slice(value, (start,) + (zero,) * (value.ndim - 1), (count, *value.shape[1:]))


def summed_share(value, axis):
    count = lax.axis_size(axis)
    rows = value.shape[0] // count
    total = rows_at(value, place(axis) * jnp.uint32(rows), rows)
    for d in range(1, count):
        total = total + shifted(rows_at(value, place(axis, d) * jnp.uint32(rows), rows), axis, d)
    return total


def joined(value, axis):
    count = lax.axis_size(axis)
    tiles = [value] + [shifted(value, axis, d) for d in range(1, count)]
    rising = [tiles[-d % count] for d in range(count)]
    rows = value.shape[0]
    start = (jnp.uint32(count) - place(axis)) * jnp.uint32(rows)
    return rows_at(jnp.concatenate(rising + rising, axis=0), start, count * rows)


def stats_kernel(at_ref, items_ref, users_ref, own_ref, out_ref):
    for b in range(8):
        scores = dot(items_ref[...], users_ref[b * BLK : (b + 1) * BLK, :], (1, 1))
        top = jnp.max(scores, axis=0, keepdims=True)
        out_ref[0, pl.ds(at_ref[b], 1), :] = top
        out_ref[0, pl.ds(8 + at_ref[b], 1), :] = jnp.sum(jnp.exp(scores - top), axis=0, keepdims=True)
    out_ref[0, 16:40, :] = own_ref[...]
    for p in range(1, 8):
        out_ref[p] = out_ref[0]


def stats(at, items, users, own):
    return pl.pallas_call(
        stats_kernel,
        in_specs=[SMEM, VMEM, VMEM, VMEM],
        out_shape=jax.ShapeDtypeStruct((8, 40, BLK), F32),
        compiler_params=pltpu.CompilerParams(vmem_limit_bytes=20 * 2**20),
        name="stats",
    )(at, items, users, own)


def users_kernel(
    at_ref, items_ref, users_ref, got_ref, all_ref, keep_ref, give_ref, turned_ref, index_ref
):
    turned_ref[...] = items_ref[...].T
    spot = lax.broadcasted_iota(jnp.int32, (ROWS, BLK), 0)
    index_ref[...] = (spot // BLK) * ROWS + spot % BLK + at_ref[8]
    for b in range(8):
        c = at_ref[b]
        tops = got_ref[:, pl.ds(c, 1), :].reshape(8, BLK)
        parts = got_ref[:, pl.ds(8 + c, 1), :].reshape(8, BLK)
        own = got_ref[pl.ds(c, 1), 16:18, :].reshape(2, BLK)
        weight = own[0:1]
        target = own[1:2].astype(jnp.int32)
        top = jnp.max(tops, axis=0, keepdims=True)
        total = top + jnp.log(jnp.sum(parts * jnp.exp(tops - top), axis=0, keepdims=True))
        total = total - jnp.log(weight)
        scores = dot(items_ref[...], users_ref[b * BLK : (b + 1) * BLK, :], (1, 1))
        share = jnp.exp(scores - total)
        dscore = jnp.where(index_ref[...] == target, share - weight, share).astype(BF16)
        all_ref[:, b * BLK : (b + 1) * BLK] = dscore
        part = dot(turned_ref[...], dscore, (1, 0))
        if b % 2 == 0:
            keep_ref[b // 2] = part
        else:
            give_ref[b // 2] = part


def user_side(at, items, users, got):
    share = jax.ShapeDtypeStruct((4, 256, BLK), F32)
    return pl.pallas_call(
        users_kernel,
        in_specs=[SMEM, VMEM, VMEM, VMEM],
        out_specs=[VMEM] * 3,
        out_shape=[jax.ShapeDtypeStruct((ROWS, ROWS), BF16), share, share],
        scratch_shapes=[pltpu.VMEM((256, ROWS), BF16), pltpu.VMEM((ROWS, BLK), jnp.int32)],
        compiler_params=pltpu.CompilerParams(vmem_limit_bytes=32 * 2**20),
        name="user_side",
    )(at, items, users, got)


def items_kernel(at_ref, all_ref, users_ref, got_ref, gi_ref, ids_ref):
    gi = dot(all_ref[...], users_ref[...], (1, 0))
    ids_ref[...] = jnp.zeros_like(ids_ref)
    for z in range(8):
        part = gi[z * BLK : (z + 1) * BLK]
        largest = jnp.maximum(jnp.max(jnp.abs(part), axis=0, keepdims=True), 1e-30)
        power = jnp.ceil(jnp.log(largest) * 1.4426950408889634)
        whole = jnp.floor(part * jnp.exp2(14.9 - power) + 0.5)
        gi_ref[z, :BLK, :] = whole.astype(jnp.int32).astype(jnp.int16)
        ids_ref[z, 4:5, :] = power
    lane = lax.broadcasted_iota(jnp.int32, (8, 128), 1) // CAP
    for y in range(4):
        row = jnp.zeros((8, 128), F32)
        for p in range(8):
            piece = got_ref[p, 24 + 8 * (y // 2) : 32 + 8 * (y // 2), 128 * (y % 2) : 128 * (y % 2) + 128]
            turn = ((p - at_ref[9]) & 7) * CAP
            row = jnp.where(lane == p, pltpu.roll(piece, turn, 1), row)
        ids_ref[:, y, :128] = row
    gi_ref[:, BLK:, :] = ids_ref[...].astype(jnp.int32).astype(jnp.int16)


def item_side(at, dscore, users, got):
    return pl.pallas_call(
        items_kernel,
        in_specs=[SMEM, VMEM, VMEM, VMEM],
        out_specs=VMEM,
        out_shape=jax.ShapeDtypeStruct((8, BLK + 8, 256), jnp.int16),
        scratch_shapes=[pltpu.VMEM((8, 8, 256), F32)],
        compiler_params=pltpu.CompilerParams(vmem_limit_bytes=22 * 2**20),
        name="item_side",
    )(at, dscore, users, got)


def tower_kernel(
    core_ref, own_ref, one_ref, two_ref, three_ref, features_ref, first_ref, second_ref,
    keep_ref, give_ref,
):
    grad_user = (own_ref[0] + one_ref[...] + two_ref[...] + three_ref[...]).astype(BF16)
    features = features_ref[...].T
    pre_act = dot(first_ref[...].T, features, (1, 0))
    hidden = jax.nn.silu(pre_act).astype(BF16)
    d_second = dot(hidden, grad_user, (1, 1))
    back_grad = dot(second_ref[...], grad_user, (1, 0))
    gate = jax.nn.sigmoid(pre_act)
    grad_pre = (back_grad * gate * (1.0 + pre_act * (1.0 - gate))).astype(BF16)
    d_first = dot(features, grad_pre, (1, 1))

    @pl.when(core_ref[0] == 0)
    def _():
        keep_ref[...] = d_first
        give_ref[...] = d_second

    @pl.when(core_ref[0] != 0)
    def _():
        keep_ref[...] = d_second
        give_ref[...] = d_first


def tower_grads(core, parts, features, w_first, w_second):
    return pl.pallas_call(
        tower_kernel,
        in_specs=[SMEM] + [VMEM] * 7,
        out_specs=[VMEM] * 2,
        out_shape=[jax.ShapeDtypeStruct((256, 256), F32)] * 2,
        compiler_params=pltpu.CompilerParams(vmem_limit_bytes=16 * 2**20),
        name="tower_grads",
    )(core, *parts, features, w_first, w_second)


def pack_kernel(parts_ref, owner_ref, rank_ref, out_ref):
    item = jnp.zeros((BLK, 256), F32)
    for z in range(8):
        power = parts_ref[z, BLK : BLK + 8, :].astype(jnp.int32).astype(F32)[4:5]
        item += parts_ref[z, :BLK, :].astype(jnp.int32).astype(F32) * jnp.exp2(power - 14.9)
    item = item.astype(BF16)
    lane = lax.broadcasted_iota(jnp.int32, (64 * 8, BLK), 0)
    halves = []
    for h in range(2):
        rank = rank_ref[...] - 8 * h
        slot = jnp.where((rank >= 0) & (rank < 8), owner_ref[...] * 8 + rank, -1)
        pick = (lane == slot).astype(F32).astype(BF16)
        halves.append(dot(pick, item, (1, 0)))
    for g in range(4):
        share = slice(64 * g, 64 * g + 64)
        both = jnp.concatenate([halves[0][:, share], halves[1][:, share]], axis=1)
        out_ref[g * 512 : (g + 1) * 512, :] = both.astype(BF16)


def pack(item, owner, rank):
    return pl.pallas_call(
        pack_kernel,
        in_specs=[VMEM] * 3,
        out_shape=jax.ShapeDtypeStruct((4 * 512, 128), BF16),
        compiler_params=pltpu.CompilerParams(vmem_limit_bytes=16 * 2**20),
        name="pack",
    )(item, owner, rank)


def table_kernel(got_ref, ids_ref, out_ref, pick_ref, kept_ref):
    both = got_ref[...].T
    value = jnp.concatenate([both[:64], both[64:]], axis=1)
    ids = ids_ref[...]
    upper = ids >> 8
    lower = ids & 255
    pick = (lax.broadcasted_iota(jnp.int32, (256, TABLE), 0) == lower).astype(F32).astype(BF16)
    pick_ref[...] = pick.T

    def step(j, carry):
        for q in range(4):
            keep = jnp.broadcast_to((upper == 4 * j + q).astype(F32), (16, TABLE)).astype(BF16)
            kept_ref[q * 64 : (q + 1) * 64, :] = value * jnp.concatenate([keep] * 4, axis=0)
        part = dot(kept_ref[...], pick_ref[...], (1, 0))
        for q in range(4):
            at = pl.multiple_of((4 * j + q) * 256, 256)
            out_ref[:, pl.ds(at, 256)] = part[q * 64 : (q + 1) * 64]
        return carry

    lax.fori_loop(0, 4, step, 0)


def table(got, ids):
    return pl.pallas_call(
        table_kernel,
        in_specs=[VMEM] * 2,
        out_shape=jax.ShapeDtypeStruct((64, TABLE), F32),
        scratch_shapes=[pltpu.VMEM((TABLE, 256), BF16), pltpu.VMEM((256, TABLE), BF16)],
        compiler_params=pltpu.CompilerParams(vmem_limit_bytes=28 * 2**20),
        name="table",
    )(got, ids)


def tower(features, w_first, w_second):
    pre_act = jnp.dot(features, w_first, preferred_element_type=F32)
    hidden = jax.nn.silu(pre_act).astype(BF16)
    return pre_act, hidden, jnp.dot(hidden, w_second, preferred_element_type=F32).astype(BF16)


def step_body(
    user_features, w_first, w_second, item_embed, example_weight, positive, item_owner, item_row
):
    features = user_features[0]
    owner = item_owner.reshape(1, BLK)
    items = to_all(item_embed[0], "z").reshape(ROWS, 256)
    pair = jnp.concatenate([features, shifted(features, "k", 1)], axis=0)
    block = jnp.concatenate([pair] + [shifted(pair, "x", d) for d in range(1, 4)], axis=0)
    _, _, users = tower(block, w_first, w_second)
    block_no = jnp.arange(8, dtype=jnp.int32)
    source = 2 * ((lax.axis_index("x") - block_no // 2) & 3) + ((block_no % 2) ^ lax.axis_index("k"))
    own_place = lax.axis_index(XK).reshape(1)
    at = jnp.concatenate([source, own_place * BLK, own_place]).astype(jnp.int32)

    member = (owner == lax.broadcasted_iota(jnp.int32, (64, 1), 0)).astype(F32)
    order = lax.broadcasted_iota(jnp.int32, (BLK, BLK), 0) < lax.broadcasted_iota(jnp.int32, (BLK, BLK), 1)
    before = dot(member.astype(BF16), order.astype(BF16), (1, 0))
    rank = jnp.sum(before * member, axis=0, keepdims=True).astype(jnp.int32)
    slot = owner * CAP + rank
    held = (slot == lax.broadcasted_iota(jnp.int32, (64 * CAP, 1), 0)).astype(jnp.int32)
    rows = jnp.sum(held * (item_row + 1), axis=1).astype(F32).reshape(64, CAP)
    rows = joined(rows, "y")
    rows = rows.reshape(2, 2, 8, 128).swapaxes(1, 2).reshape(16, BLK)
    own = jnp.concatenate(
        [example_weight, positive.astype(F32), jnp.zeros((6, BLK), F32), rows], axis=0
    )
    got = exchange(stats(at, items, users, own), XK)
    dscore, keep, give = user_side(at, items, users, got)
    swapped = shifted(give, "k", 1)
    gi = item_side(at, dscore, users, got)
    gi = exchange(gi, "z")
    gu = keep + swapped
    parts = [gu] + [shifted(gu[d], "x", -d) for d in range(1, 4)]
    gu = keep + swapped
    parts = [gu] + [shifted(gu[d], "x", -d) for d in range(1, 4)]
    scale = jnp.exp2(gi[:, BLK + 4, 0].astype(F32) - 15.0)
    item = sum(gi[z, :BLK].astype(F32) * scale[z] for z in range(8)).astype(BF16)
    ids = gi[:, BLK : BLK + 4, :128].astype(jnp.int32) - 1
    ids = ids.swapaxes(0, 1).reshape(4 * 64, CAP)
    ids = jnp.concatenate([ids[:, :8].reshape(1, -1), ids[:, 8:].reshape(1, -1)], axis=1)

    core = lax.axis_index("k").astype(jnp.int32).reshape(1)
    both, other = tower_grads(core, parts, features, w_first, w_second)
    both = both + shifted(other, "k", 1)
    both = summed_share(both, "y")
    both = summed_share(both, "x")
    both = both + lax.ppermute(both, "z", [(i, i ^ 1) for i in range(8)])
    both = both + sum(lax.ppermute(both, "z", [(i, i ^ step) for i in range(8)]) for step in (2, 4, 6))

    send = pack(gi, owner, rank).reshape(256, 8, 128)
    came = exchange(send, YZXK).reshape(256 * 8, 128)
    both = to_all(both, KYX).reshape(512, 256)
    grad_table = table(came, ids).T
    return both[:256], both[256:], grad_table


def solution(mesh):
    torus = Mesh(mesh.devices.reshape(8, 4, 2, mesh.shape["grp"]), ("z", "x", "k", "y"))
    rows = ("z", "x", "k")
    placed = (
        P("y", rows, None),
        P(),
        P(),
        P("y", rows, None),
        P("y", rows),
        P("y", rows),
        P("y", rows, None),
        P("y", rows),
    )
    return jax.shard_map(step_body, mesh=torus, in_specs=placed, out_specs=(P(), P(), P(rows, "y")), check_vma=False)
```

```python
import jax
import jax.numpy as jnp
from jax import lax
from jax.experimental import pallas as pl
from jax.experimental.pallas import tpu as pltpu
from jax.sharding import Mesh
from jax.sharding import PartitionSpec as P

TABLE = 4096
CAP = 16
BLK = 256
ROWS = 8 * BLK
XK = ("x", "k")
YX = ("y", "x")
YZXK = ("y", "z", "x", "k")
F32 = jnp.float32
BF16 = jnp.bfloat16
VMEM = pl.BlockSpec(memory_space=pltpu.VMEM)
SMEM = pl.BlockSpec(memory_space=pltpu.SMEM)


def dot(left, right, dims):
    return lax.dot_general(left, right, ((dims[0:1], dims[1:2]), ((), ())), preferred_element_type=F32)


def exchange(value, axes):
    return lax.all_to_all(value, axes, 0, 0, tiled=True)


def to_all(value, axes):
    return exchange(jnp.broadcast_to(value[None], (lax.axis_size(axes), *value.shape)), axes)


def shifted(value, axis, step):
    count = lax.axis_size(axis)
    return lax.ppermute(value, axis, [(i, (i + step) % count) for i in range(count)])


def place(axis, step=0):
    return (lax.axis_index(axis).astype(jnp.uint32) + jnp.uint32(step)) & jnp.uint32(lax.axis_size(axis) - 1)


def rows_at(value, start, count):
    zero = jnp.uint32(0)
    return lax.dynamic_slice(value, (start,) + (zero,) * (value.ndim - 1), (count, *value.shape[1:]))


def summed_share(value, axis):
    count = lax.axis_size(axis)
    rows = value.shape[0] // count
    total = rows_at(value, place(axis) * jnp.uint32(rows), rows)
    for d in range(1, count):
        total = total + shifted(rows_at(value, place(axis, d) * jnp.uint32(rows), rows), axis, d)
    return total


def joined(value, axis):
    count = lax.axis_size(axis)
    tiles = [value] + [shifted(value, axis, d) for d in range(1, count)]
    rising = [tiles[-d % count] for d in range(count)]
    rows = value.shape[0]
    start = (jnp.uint32(count) - place(axis)) * jnp.uint32(rows)
    return rows_at(jnp.concatenate(rising + rising, axis=0), start, count * rows)


def stats_kernel(at_ref, items_ref, users_ref, own_ref, out_ref):
    for b in range(8):
        scores = dot(items_ref[...], users_ref[b * BLK : (b + 1) * BLK, :], (1, 1))
        top = jnp.max(scores, axis=0, keepdims=True)
        part = top + jnp.log(jnp.sum(jnp.exp(scores - top), axis=0, keepdims=True))
        out_ref[0, pl.ds(at_ref[b], 1), :] = part
    for p in range(1, 8):
        out_ref[p, :8, :] = out_ref[0, :8, :]
    for p in range(8):
        out_ref[p, 8:16, :] = own_ref[p]


def stats(at, items, users, own):
    return pl.pallas_call(
        stats_kernel,
        in_specs=[SMEM, VMEM, VMEM, VMEM],
        out_specs=VMEM,
        out_shape=jax.ShapeDtypeStruct((8, 16, BLK), F32),
        compiler_params=pltpu.CompilerParams(vmem_limit_bytes=20 * 2**20),
        name="stats",
    )(at, items, users, own)


def users_kernel(
    at_ref, items_ref, users_ref, got_ref, all_ref, keep_ref, give_ref, turned_ref, index_ref
):
    turned_ref[...] = items_ref[...].T
    spot = lax.broadcasted_iota(jnp.int32, (ROWS, BLK), 0)
    index_ref[...] = (spot // BLK) * ROWS + spot % BLK + at_ref[8]
    for b in range(8):
        c = at_ref[b]
        tops = got_ref[:, pl.ds(c, 1), :].reshape(8, BLK)
        own = got_ref[pl.ds(c, 1), 8:10, :].reshape(2, BLK)
        weight = own[0:1]
        target = own[1:2].astype(jnp.int32)
        top = jnp.max(tops, axis=0, keepdims=True)
        total = top + jnp.log(jnp.sum(jnp.exp(tops - top), axis=0, keepdims=True))
        total = total - jnp.log(weight)
        scores = dot(items_ref[...], users_ref[b * BLK : (b + 1) * BLK, :], (1, 1))
        share = jnp.exp(scores - total)
        dscore = jnp.where(index_ref[...] == target, share - weight, share).astype(BF16)
        all_ref[:, b * BLK : (b + 1) * BLK] = dscore
        part = dot(turned_ref[...], dscore, (1, 0))
        if b % 2 == 0:
            keep_ref[b // 2] = part
        else:
            give_ref[b // 2] = part


def user_side(at, items, users, got):
    share = jax.ShapeDtypeStruct((4, 256, BLK), F32)
    return pl.pallas_call(
        users_kernel,
        in_specs=[SMEM, VMEM, VMEM, VMEM],
        out_specs=[VMEM] * 3,
        out_shape=[jax.ShapeDtypeStruct((ROWS, ROWS), BF16), share, share],
        scratch_shapes=[pltpu.VMEM((256, ROWS), BF16), pltpu.VMEM((ROWS, BLK), jnp.int32)],
        compiler_params=pltpu.CompilerParams(vmem_limit_bytes=32 * 2**20),
        name="user_side",
    )(at, items, users, got)


def items_kernel(all_ref, users_ref, got_ref, gi_ref, ids_ref):
    gi = dot(all_ref[...], users_ref[...], (1, 0))
    ids_ref[...] = jnp.zeros_like(ids_ref)
    for z in range(8):
        part = gi[z * BLK : (z + 1) * BLK]
        largest = jnp.maximum(jnp.max(jnp.abs(part), axis=0, keepdims=True), 1e-30)
        power = jnp.ceil(jnp.log(largest) * 1.4426950408889634)
        whole = jnp.floor(part * jnp.exp2(14.9 - power) + 0.5)
        gi_ref[z, :BLK, :] = whole.astype(jnp.int32).astype(jnp.int16)
        ids_ref[z, 4:5, :] = power
    lane = lax.broadcasted_iota(jnp.int32, (8, 128), 1) // CAP
    line = lax.broadcasted_iota(jnp.int32, (8, 128), 0)
    for y in range(4):
        row = jnp.zeros((8, 128), F32)
        for p in range(8):
            piece = got_ref[p, 10 + y // 2 : 11 + y // 2, 128 * (y % 2) : 128 * (y % 2) + 128]
            piece = jnp.broadcast_to(piece, (8, 128))
            for z in range(8):
                turn = (p - z) % 8 * CAP
                row = jnp.where((lane == p) & (line == z), pltpu.roll(piece, turn, 1) if turn else piece, row)
        ids_ref[:, y, :128] = row
    gi_ref[:, BLK:, :] = ids_ref[...].astype(jnp.int32).astype(jnp.int16)


def item_side(dscore, users, got):
    return pl.pallas_call(
        items_kernel,
        in_specs=[VMEM, VMEM, VMEM],
        out_specs=VMEM,
        out_shape=jax.ShapeDtypeStruct((8, BLK + 8, 256), jnp.int16),
        scratch_shapes=[pltpu.VMEM((8, 8, 256), F32)],
        compiler_params=pltpu.CompilerParams(vmem_limit_bytes=22 * 2**20),
        name="item_side",
    )(dscore, users, got)


def tower_kernel(
    core_ref, own_ref, one_ref, two_ref, three_ref, features_ref, first_ref, second_ref,
    keep_ref, give_ref,
):
    grad_user = (own_ref[0] + one_ref[...] + two_ref[...] + three_ref[...]).astype(BF16)
    features = features_ref[...].T
    pre_act = dot(first_ref[...].T, features, (1, 0))
    hidden = jax.nn.silu(pre_act).astype(BF16)
    d_second = dot(hidden, grad_user, (1, 1))
    back_grad = dot(second_ref[...], grad_user, (1, 0))
    gate = jax.nn.sigmoid(pre_act)
    grad_pre = (back_grad * gate * (1.0 + pre_act * (1.0 - gate))).astype(BF16)
    d_first = dot(features, grad_pre, (1, 1))

    @pl.when(core_ref[0] == 0)
    def _():
        keep_ref[...] = d_first
        give_ref[...] = d_second

    @pl.when(core_ref[0] != 0)
    def _():
        keep_ref[...] = d_second
        give_ref[...] = d_first


def tower_grads(core, parts, features, w_first, w_second):
    return pl.pallas_call(
        tower_kernel,
        in_specs=[SMEM] + [VMEM] * 7,
        out_specs=[VMEM] * 2,
        out_shape=[jax.ShapeDtypeStruct((256, 256), F32)] * 2,
        compiler_params=pltpu.CompilerParams(vmem_limit_bytes=16 * 2**20),
        name="tower_grads",
    )(core, *parts, features, w_first, w_second)


def pack_kernel(parts_ref, owner_ref, rank_ref, out_ref):
    item = jnp.zeros((BLK, 256), F32)
    for z in range(8):
        power = parts_ref[z, BLK : BLK + 8, :].astype(jnp.int32).astype(F32)[4:5]
        item += parts_ref[z, :BLK, :].astype(jnp.int32).astype(F32) * jnp.exp2(power - 14.9)
    item = item.astype(BF16)
    lane = lax.broadcasted_iota(jnp.int32, (64 * 8, BLK), 0)
    halves = []
    for h in range(2):
        rank = rank_ref[...] - 8 * h
        slot = jnp.where((rank >= 0) & (rank < 8), owner_ref[...] * 8 + rank, -1)
        pick = (lane == slot).astype(F32).astype(BF16)
        halves.append(dot(pick, item, (1, 0)))
    for g in range(4):
        share = slice(64 * g, 64 * g + 64)
        both = jnp.concatenate([halves[0][:, share], halves[1][:, share]], axis=1)
        out_ref[g * 512 : (g + 1) * 512, :] = both.astype(BF16)


def pack(item, owner, rank):
    return pl.pallas_call(
        pack_kernel,
        in_specs=[VMEM] * 3,
        out_shape=jax.ShapeDtypeStruct((4 * 512, 128), BF16),
        compiler_params=pltpu.CompilerParams(vmem_limit_bytes=16 * 2**20),
        name="pack",
    )(item, owner, rank)


def table_kernel(got_ref, ids_ref, out_ref, pick_ref, kept_ref):
    both = got_ref[...].T
    value = jnp.concatenate([both[:64], both[64:]], axis=1)
    ids = ids_ref[...]
    upper = ids >> 8
    lower = ids & 255
    pick = (lax.broadcasted_iota(jnp.int32, (256, TABLE), 0) == lower).astype(F32).astype(BF16)
    pick_ref[...] = pick.T

    def step(j, carry):
        for q in range(4):
            keep = jnp.broadcast_to((upper == 4 * j + q).astype(F32), (16, TABLE)).astype(BF16)
            kept_ref[q * 64 : (q + 1) * 64, :] = value * jnp.concatenate([keep] * 4, axis=0)
        part = dot(kept_ref[...], pick_ref[...], (1, 0))
        for q in range(4):
            at = pl.multiple_of((4 * j + q) * 256, 256)
            out_ref[:, pl.ds(at, 256)] = part[q * 64 : (q + 1) * 64]
        return carry

    lax.fori_loop(0, 4, step, 0)


def table(got, ids):
    return pl.pallas_call(
        table_kernel,
        in_specs=[VMEM] * 2,
        out_shape=jax.ShapeDtypeStruct((64, TABLE), F32),
        scratch_shapes=[pltpu.VMEM((TABLE, 256), BF16), pltpu.VMEM((256, TABLE), BF16)],
        compiler_params=pltpu.CompilerParams(vmem_limit_bytes=28 * 2**20),
        name="table",
    )(got, ids)


def tower(features, w_first, w_second):
    pre_act = jnp.dot(features, w_first, preferred_element_type=F32)
    hidden = jax.nn.silu(pre_act).astype(BF16)
    return pre_act, hidden, jnp.dot(hidden, w_second, preferred_element_type=F32).astype(BF16)


def step_body(
    user_features, w_first, w_second, item_embed, example_weight, positive, item_owner, item_row
):
    features = user_features[0]
    owner = item_owner.reshape(1, BLK)
    items = to_all(item_embed[0], "z").reshape(ROWS, 256)
    pair = jnp.concatenate([features, shifted(features, "k", 1)], axis=0)
    block = jnp.concatenate([pair] + [shifted(pair, "x", d) for d in range(1, 4)], axis=0)
    _, _, users = tower(block, w_first, w_second)
    block_no = jnp.arange(8, dtype=jnp.int32)
    source = 2 * ((lax.axis_index("x") - block_no // 2) & 3) + ((block_no % 2) ^ lax.axis_index("k"))
    own_place = lax.axis_index(XK).reshape(1)
    at = jnp.concatenate([source, own_place * BLK]).astype(jnp.int32)

    member = (owner == lax.broadcasted_iota(jnp.int32, (64, 1), 0)).astype(F32)
    order = lax.broadcasted_iota(jnp.int32, (BLK, BLK), 0) < lax.broadcasted_iota(jnp.int32, (BLK, BLK), 1)
    before = dot(member.astype(BF16), order.astype(BF16), (1, 0))
    rank = jnp.sum(before * member, axis=0, keepdims=True).astype(jnp.int32)
    slot = owner * CAP + rank
    held = (slot == lax.broadcasted_iota(jnp.int32, (64 * CAP, 1), 0)).astype(jnp.int32)
    rows = jnp.sum(held * (item_row + 1), axis=1).astype(F32).reshape(64, CAP)
    rows = joined(rows, "y")
    rows = rows.reshape(4, 8, 8, CAP).transpose(2, 0, 1, 3).reshape(8, 2, BLK)
    own = jnp.concatenate([example_weight, positive.astype(F32)], axis=0)
    own = jnp.concatenate(
        [jnp.broadcast_to(own[None], (8, 2, BLK)), rows, jnp.zeros((8, 4, BLK), F32)], axis=1
    )
    got = exchange(stats(at, items, users, own), XK)
    dscore, keep, give = user_side(at, items, users, got)
    swapped = shifted(give, "k", 1)
    gi = item_side(dscore, users, got)
    gi = exchange(gi, "z")
    gu = keep + swapped
    parts = [gu] + [shifted(gu[d], "x", -d) for d in range(1, 4)]
    gu = keep + swapped
    parts = [gu] + [shifted(gu[d], "x", -d) for d in range(1, 4)]
    scale = jnp.exp2(gi[:, BLK + 4, 0].astype(F32) - 15.0)
    item = sum(gi[z, :BLK].astype(F32) * scale[z] for z in range(8)).astype(BF16)
    ids = gi[:, BLK : BLK + 4, :128].astype(jnp.int32) - 1
    ids = ids.swapaxes(0, 1).reshape(4 * 64, CAP)
    ids = jnp.concatenate([ids[:, :8].reshape(1, -1), ids[:, 8:].reshape(1, -1)], axis=1)

    core = lax.axis_index("k").astype(jnp.int32).reshape(1)
    both, other = tower_grads(core, parts, features, w_first, w_second)
    both = both + shifted(other, "k", 1)
    both = summed_share(both, "y")
    both = summed_share(both, "x")
    both = both + lax.ppermute(both, "z", [(i, i ^ 1) for i in range(8)])
    both = both + sum(lax.ppermute(both, "z", [(i, i ^ step) for i in range(8)]) for step in (2, 4, 6))

    send = pack(gi, owner, rank).reshape(256, 8, 128)
    came = exchange(send, YZXK).reshape(256 * 8, 128)
    both = to_all(both, YX).reshape(256, 256)
    grad_table = table(came, ids).T
    other = shifted(both, "k", 1)
    first = lax.axis_index("k") == 0
    return jnp.where(first, both, other), jnp.where(first, other, both), grad_table


def solution(mesh):
    torus = Mesh(mesh.devices.reshape(8, 4, 2, mesh.shape["grp"]), ("z", "x", "k", "y"))
    rows = ("z", "x", "k")
    placed = (
        P("y", rows, None),
        P(),
        P(),
        P("y", rows, None),
        P("y", rows),
        P("y", rows),
        P("y", rows, None),
        P("y", rows),
    )
    return jax.shard_map(step_body, mesh=torus, in_specs=placed, out_specs=(P(), P(), P(rows, "y")), check_vma=False)
```

```python
import jax
import jax.numpy as jnp
from jax import lax
from jax.experimental import pallas as pl
from jax.experimental.pallas import tpu as pltpu
from jax.sharding import Mesh
from jax.sharding import PartitionSpec as P

TABLE = 4096
CAP = 16
BLK = 256
ROWS = 8 * BLK
XK = ("x", "k")
YX = ("y", "x")
YZXK = ("y", "z", "x", "k")
F32 = jnp.float32
BF16 = jnp.bfloat16
VMEM = pl.BlockSpec(memory_space=pltpu.VMEM)
SMEM = pl.BlockSpec(memory_space=pltpu.SMEM)


def dot(left, right, dims):
    return lax.dot_general(left, right, ((dims[0:1], dims[1:2]), ((), ())), preferred_element_type=F32)


def exchange(value, axes):
    return lax.all_to_all(value, axes, 0, 0, tiled=True)


def to_all(value, axes):
    return exchange(jnp.broadcast_to(value[None], (lax.axis_size(axes), *value.shape)), axes)


def shifted(value, axis, step):
    count = lax.axis_size(axis)
    return lax.ppermute(value, axis, [(i, (i + step) % count) for i in range(count)])


def place(axis, step=0):
    return (lax.axis_index(axis).astype(jnp.uint32) + jnp.uint32(step)) & jnp.uint32(lax.axis_size(axis) - 1)


def rows_at(value, start, count):
    zero = jnp.uint32(0)
    return lax.dynamic_slice(value, (start,) + (zero,) * (value.ndim - 1), (count, *value.shape[1:]))


def summed_share(value, axis):
    count = lax.axis_size(axis)
    rows = value.shape[0] // count
    total = rows_at(value, place(axis) * jnp.uint32(rows), rows)
    for d in range(1, count):
        total = total + shifted(rows_at(value, place(axis, d) * jnp.uint32(rows), rows), axis, d)
    return total


def joined(value, axis):
    count = lax.axis_size(axis)
    tiles = [value] + [shifted(value, axis, d) for d in range(1, count)]
    rising = [tiles[-d % count] for d in range(count)]
    rows = value.shape[0]
    start = (jnp.uint32(count) - place(axis)) * jnp.uint32(rows)
    return rows_at(jnp.concatenate(rising + rising, axis=0), start, count * rows)


def stats_kernel(at_ref, items_ref, users_ref, own_ref, out_ref):
    for b in range(8):
        scores = dot(items_ref[...], users_ref[b * BLK : (b + 1) * BLK, :], (1, 1))
        top = jnp.max(scores, axis=0, keepdims=True)
        part = top + jnp.log(jnp.sum(jnp.exp(scores - top), axis=0, keepdims=True))
        out_ref[0, pl.ds(at_ref[b], 1), :] = part
    for p in range(1, 8):
        out_ref[p, :8, :] = out_ref[0, :8, :]
    for p in range(8):
        out_ref[p, 8:16, :] = own_ref[p]


def stats(at, items, users, own):
    return pl.pallas_call(
        stats_kernel,
        in_specs=[SMEM, VMEM, VMEM, VMEM],
        out_specs=VMEM,
        out_shape=jax.ShapeDtypeStruct((8, 16, BLK), F32),
        compiler_params=pltpu.CompilerParams(vmem_limit_bytes=20 * 2**20),
        name="stats",
    )(at, items, users, own)


def users_kernel(
    at_ref, items_ref, users_ref, got_ref, all_ref, keep_ref, give_ref, turned_ref, index_ref
):
    turned_ref[...] = items_ref[...].T
    spot = lax.broadcasted_iota(jnp.int32, (ROWS, BLK), 0)
    index_ref[...] = (spot // BLK) * ROWS + spot % BLK + at_ref[8]
    for b in range(8):
        c = at_ref[b]
        tops = got_ref[:, pl.ds(c, 1), :].reshape(8, BLK)
        own = got_ref[pl.ds(c, 1), 8:10, :].reshape(2, BLK)
        weight = own[0:1]
        target = own[1:2].astype(jnp.int32)
        top = jnp.max(tops, axis=0, keepdims=True)
        total = top + jnp.log(jnp.sum(jnp.exp(tops - top), axis=0, keepdims=True))
        total = total - jnp.log(weight)
        scores = dot(items_ref[...], users_ref[b * BLK : (b + 1) * BLK, :], (1, 1))
        share = jnp.exp(scores - total)
        dscore = jnp.where(index_ref[...] == target, share - weight, share).astype(BF16)
        all_ref[:, b * BLK : (b + 1) * BLK] = dscore
        part = dot(turned_ref[...], dscore, (1, 0))
        if b % 2 == 0:
            keep_ref[b // 2] = part
        else:
            give_ref[b // 2] = part


def user_side(at, items, users, got):
    share = jax.ShapeDtypeStruct((4, 256, BLK), F32)
    return pl.pallas_call(
        users_kernel,
        in_specs=[SMEM, VMEM, VMEM, VMEM],
        out_specs=[VMEM] * 3,
        out_shape=[jax.ShapeDtypeStruct((ROWS, ROWS), BF16), share, share],
        scratch_shapes=[pltpu.VMEM((256, ROWS), BF16), pltpu.VMEM((ROWS, BLK), jnp.int32)],
        compiler_params=pltpu.CompilerParams(vmem_limit_bytes=32 * 2**20),
        name="user_side",
    )(at, items, users, got)


def items_kernel(all_ref, users_ref, got_ref, gi_ref, ids_ref):
    gi = dot(all_ref[...], users_ref[...], (1, 0))
    ids_ref[...] = jnp.zeros_like(ids_ref)
    for z in range(8):
        part = gi[z * BLK : (z + 1) * BLK]
        largest = jnp.maximum(jnp.max(jnp.abs(part), axis=0, keepdims=True), 1e-30)
        power = jnp.ceil(jnp.log(largest) * 1.4426950408889634)
        whole = jnp.floor(part * jnp.exp2(14.9 - power) + 0.5)
        gi_ref[z, :BLK, :] = whole.astype(jnp.int32).astype(jnp.int16)
        ids_ref[z, 4:5, :] = power
    lane = lax.broadcasted_iota(jnp.int32, (8, 128), 1) // CAP
    line = lax.broadcasted_iota(jnp.int32, (8, 128), 0)
    for y in range(4):
        row = jnp.zeros((8, 128), F32)
        for p in range(8):
            piece = got_ref[p, 10 + y // 2 : 11 + y // 2, 128 * (y % 2) : 128 * (y % 2) + 128]
            piece = jnp.broadcast_to(piece, (8, 128))
            for z in range(8):
                turn = (p - z) % 8 * CAP
                row = jnp.where((lane == p) & (line == z), pltpu.roll(piece, turn, 1) if turn else piece, row)
        ids_ref[:, y, :128] = row
    gi_ref[:, BLK:, :] = ids_ref[...].astype(jnp.int32).astype(jnp.int16)


def item_side(dscore, users, got):
    return pl.pallas_call(
        items_kernel,
        in_specs=[VMEM, VMEM, VMEM],
        out_specs=VMEM,
        out_shape=jax.ShapeDtypeStruct((8, BLK + 8, 256), jnp.int16),
        scratch_shapes=[pltpu.VMEM((8, 8, 256), F32)],
        compiler_params=pltpu.CompilerParams(vmem_limit_bytes=22 * 2**20),
        name="item_side",
    )(dscore, users, got)


def tower_kernel(
    core_ref, own_ref, one_ref, two_ref, three_ref, features_ref, first_ref, second_ref,
    keep_ref, give_ref,
):
    grad_user = (own_ref[0] + one_ref[...] + two_ref[...] + three_ref[...]).astype(BF16)
    features = features_ref[...].T
    pre_act = dot(first_ref[...].T, features, (1, 0))
    hidden = jax.nn.silu(pre_act).astype(BF16)
    d_second = dot(hidden, grad_user, (1, 1))
    back_grad = dot(second_ref[...], grad_user, (1, 0))
    gate = jax.nn.sigmoid(pre_act)
    grad_pre = (back_grad * gate * (1.0 + pre_act * (1.0 - gate))).astype(BF16)
    d_first = dot(features, grad_pre, (1, 1))

    @pl.when(core_ref[0] == 0)
    def _():
        keep_ref[...] = d_first
        give_ref[...] = d_second

    @pl.when(core_ref[0] != 0)
    def _():
        keep_ref[...] = d_second
        give_ref[...] = d_first


def tower_grads(core, parts, features, w_first, w_second):
    return pl.pallas_call(
        tower_kernel,
        in_specs=[SMEM] + [VMEM] * 7,
        out_specs=[VMEM] * 2,
        out_shape=[jax.ShapeDtypeStruct((256, 256), F32)] * 2,
        compiler_params=pltpu.CompilerParams(vmem_limit_bytes=16 * 2**20),
        name="tower_grads",
    )(core, *parts, features, w_first, w_second)


def pack_kernel(parts_ref, owner_ref, rank_ref, out_ref):
    item = jnp.zeros((BLK, 256), F32)
    for z in range(8):
        power = parts_ref[z, BLK : BLK + 8, :].astype(jnp.int32).astype(F32)[4:5]
        item += parts_ref[z, :BLK, :].astype(jnp.int32).astype(F32) * jnp.exp2(power - 14.9)
    item = item.astype(BF16)
    lane = lax.broadcasted_iota(jnp.int32, (64 * 8, BLK), 0)
    halves = []
    for h in range(2):
        rank = rank_ref[...] - 8 * h
        slot = jnp.where((rank >= 0) & (rank < 8), owner_ref[...] * 8 + rank, -1)
        pick = (lane == slot).astype(F32).astype(BF16)
        halves.append(dot(pick, item, (1, 0)))
    for g in range(4):
        share = slice(64 * g, 64 * g + 64)
        both = jnp.concatenate([halves[0][:, share], halves[1][:, share]], axis=1)
        out_ref[g * 512 : (g + 1) * 512, :] = both.astype(BF16)


def pack(item, owner, rank):
    return pl.pallas_call(
        pack_kernel,
        in_specs=[VMEM] * 3,
        out_shape=jax.ShapeDtypeStruct((4 * 512, 128), BF16),
        compiler_params=pltpu.CompilerParams(vmem_limit_bytes=16 * 2**20),
        name="pack",
    )(item, owner, rank)


def table_kernel(got_ref, ids_ref, out_ref, pick_ref, kept_ref):
    both = got_ref[...].T
    value = jnp.concatenate([both[:64], both[64:]], axis=1)
    ids = ids_ref[...]
    upper = ids >> 8
    lower = ids & 255
    pick = (lax.broadcasted_iota(jnp.int32, (256, TABLE), 0) == lower).astype(F32).astype(BF16)
    pick_ref[...] = pick.T

    def step(j, carry):
        for q in range(4):
            keep = jnp.broadcast_to((upper == 4 * j + q).astype(F32), (16, TABLE)).astype(BF16)
            kept_ref[q * 64 : (q + 1) * 64, :] = value * jnp.concatenate([keep] * 4, axis=0)
        part = dot(kept_ref[...], pick_ref[...], (1, 0))
        for q in range(4):
            at = pl.multiple_of((4 * j + q) * 256, 256)
            out_ref[:, pl.ds(at, 256)] = part[q * 64 : (q + 1) * 64]
        return carry

    lax.fori_loop(0, 4, step, 0)


def table(got, ids):
    return pl.pallas_call(
        table_kernel,
        in_specs=[VMEM] * 2,
        out_shape=jax.ShapeDtypeStruct((64, TABLE), F32),
        scratch_shapes=[pltpu.VMEM((TABLE, 256), BF16), pltpu.VMEM((256, TABLE), BF16)],
        compiler_params=pltpu.CompilerParams(vmem_limit_bytes=28 * 2**20),
        name="table",
    )(got, ids)


def tower(features, w_first, w_second):
    pre_act = jnp.dot(features, w_first, preferred_element_type=F32)
    hidden = jax.nn.silu(pre_act).astype(BF16)
    return pre_act, hidden, jnp.dot(hidden, w_second, preferred_element_type=F32).astype(BF16)


def step_body(
    user_features, w_first, w_second, item_embed, example_weight, positive, item_owner, item_row
):
    features = user_features[0]
    owner = item_owner.reshape(1, BLK)
    items = to_all(item_embed[0], "z").reshape(ROWS, 256)
    pair = jnp.concatenate([features, shifted(features, "k", 1)], axis=0)
    block = jnp.concatenate([pair] + [shifted(pair, "x", d) for d in range(1, 4)], axis=0)
    _, _, users = tower(block, w_first, w_second)
    block_no = jnp.arange(8, dtype=jnp.int32)
    source = 2 * ((lax.axis_index("x") - block_no // 2) & 3) + ((block_no % 2) ^ lax.axis_index("k"))
    own_place = lax.axis_index(XK).reshape(1)
    at = jnp.concatenate([source, own_place * BLK]).astype(jnp.int32)

    member = (owner == lax.broadcasted_iota(jnp.int32, (64, 1), 0)).astype(F32)
    order = lax.broadcasted_iota(jnp.int32, (BLK, BLK), 0) < lax.broadcasted_iota(jnp.int32, (BLK, BLK), 1)
    before = dot(member.astype(BF16), order.astype(BF16), (1, 0))
    rank = jnp.sum(before * member, axis=0, keepdims=True).astype(jnp.int32)
    slot = owner * CAP + rank
    held = (slot == lax.broadcasted_iota(jnp.int32, (64 * CAP, 1), 0)).astype(jnp.int32)
    rows = jnp.sum(held * (item_row + 1), axis=1).astype(F32).reshape(64, CAP)
    rows = joined(rows, "y")
    rows = rows.reshape(4, 8, 8, CAP).transpose(2, 0, 1, 3).reshape(8, 2, BLK)
    own = jnp.concatenate([example_weight, positive.astype(F32)], axis=0)
    own = jnp.concatenate(
        [jnp.broadcast_to(own[None], (8, 2, BLK)), rows, jnp.zeros((8, 4, BLK), F32)], axis=1
    )
    got = exchange(stats(at, items, users, own), XK)
    dscore, keep, give = user_side(at, items, users, got)
    swapped = shifted(give, "k", 1)
    gi = item_side(dscore, users, got)
    gi = exchange(gi, "z")
    gu = keep + swapped
    parts = [gu] + [shifted(gu[d], "x", -d) for d in range(1, 4)]
    gu = keep + swapped
    parts = [gu] + [shifted(gu[d], "x", -d) for d in range(1, 4)]
    scale = jnp.exp2(gi[:, BLK + 4, 0].astype(F32) - 15.0)
    item = sum(gi[z, :BLK].astype(F32) * scale[z] for z in range(8)).astype(BF16)
    ids = gi[:, BLK : BLK + 4, :128].astype(jnp.int32) - 1
    ids = ids.swapaxes(0, 1).reshape(4 * 64, CAP)
    ids = jnp.concatenate([ids[:, :8].reshape(1, -1), ids[:, 8:].reshape(1, -1)], axis=1)

    core = lax.axis_index("k").astype(jnp.int32).reshape(1)
    both, other = tower_grads(core, parts, features, w_first, w_second)
    both = both + shifted(other, "k", 1)
    both = summed_share(both, "y")
    both = summed_share(both, "x")
    for step in (1, 2, 4):
        both = both + lax.ppermute(both, "z", [(i, i ^ step) for i in range(8)])

    send = pack(gi, owner, rank).reshape(256, 8, 128)
    came = exchange(send, YZXK).reshape(256 * 8, 128)
    both = to_all(both, YX).reshape(256, 256)
    grad_table = table(came, ids).T
    other = shifted(both, "k", 1)
    first = lax.axis_index("k") == 0
    return jnp.where(first, both, other), jnp.where(first, other, both), grad_table


def solution(mesh):
    torus = Mesh(mesh.devices.reshape(8, 4, 2, mesh.shape["grp"]), ("z", "x", "k", "y"))
    rows = ("z", "x", "k")
    placed = (
        P("y", rows, None),
        P(),
        P(),
        P("y", rows, None),
        P("y", rows),
        P("y", rows),
        P("y", rows, None),
        P("y", rows),
    )
    return jax.shard_map(
        step_body, mesh=torus, in_specs=placed, out_specs=(P(), P(), P(rows, "y")), check_vma=False
    )
```

```python
import jax
import jax.numpy as jnp
from jax import lax
from jax.experimental import pallas as pl
from jax.experimental.pallas import tpu as pltpu
from jax.sharding import Mesh
from jax.sharding import PartitionSpec as P

TABLE = 4096
CAP = 16
BLK = 256
ROWS = 8 * BLK
XK = ("x", "k")
YX = ("y", "x")
YZXK = ("y", "z", "x", "k")
F32 = jnp.float32
BF16 = jnp.bfloat16
VMEM = pl.BlockSpec(memory_space=pltpu.VMEM)
SMEM = pl.BlockSpec(memory_space=pltpu.SMEM)


def dot(left, right, dims):
    return lax.dot_general(left, right, ((dims[0:1], dims[1:2]), ((), ())), preferred_element_type=F32)


def exchange(value, axes):
    return lax.all_to_all(value, axes, 0, 0, tiled=True)


def to_all(value, axes):
    return exchange(jnp.broadcast_to(value[None], (lax.axis_size(axes), *value.shape)), axes)


def shifted(value, axis, step):
    count = lax.axis_size(axis)
    return lax.ppermute(value, axis, [(i, (i + step) % count) for i in range(count)])


def place(axis, step=0):
    return (lax.axis_index(axis).astype(jnp.uint32) + jnp.uint32(step)) & jnp.uint32(lax.axis_size(axis) - 1)


def rows_at(value, start, count):
    zero = jnp.uint32(0)
    return lax.dynamic_slice(value, (start,) + (zero,) * (value.ndim - 1), (count, *value.shape[1:]))


def summed_share(value, axis):
    count = lax.axis_size(axis)
    rows = value.shape[0] // count
    total = rows_at(value, place(axis) * jnp.uint32(rows), rows)
    for d in range(1, count):
        total = total + shifted(rows_at(value, place(axis, d) * jnp.uint32(rows), rows), axis, d)
    return total


def joined(value, axis):
    count = lax.axis_size(axis)
    tiles = [value] + [shifted(value, axis, d) for d in range(1, count)]
    rising = [tiles[-d % count] for d in range(count)]
    rows = value.shape[0]
    start = (jnp.uint32(count) - place(axis)) * jnp.uint32(rows)
    return rows_at(jnp.concatenate(rising + rising, axis=0), start, count * rows)


def stats_kernel(at_ref, items_ref, users_ref, own_ref, out_ref):
    for b in range(8):
        scores = dot(items_ref[...], users_ref[b * BLK : (b + 1) * BLK, :], (1, 1))
        top = jnp.max(scores, axis=0, keepdims=True)
        part = top + jnp.log(jnp.sum(jnp.exp(scores - top), axis=0, keepdims=True))
        out_ref[0, pl.ds(at_ref[b], 1), :] = part
    for p in range(1, 8):
        out_ref[p, :8, :] = out_ref[0, :8, :]
    for p in range(8):
        out_ref[p, 8:16, :] = own_ref[p]


def stats(at, items, users, own):
    return pl.pallas_call(
        stats_kernel,
        in_specs=[SMEM, VMEM, VMEM, VMEM],
        out_specs=VMEM,
        out_shape=jax.ShapeDtypeStruct((8, 16, BLK), F32),
        compiler_params=pltpu.CompilerParams(vmem_limit_bytes=20 * 2**20),
        name="stats",
    )(at, items, users, own)


def users_kernel(
    at_ref, items_ref, users_ref, got_ref, all_ref, keep_ref, give_ref, turned_ref, index_ref
):
    turned_ref[...] = items_ref[...].T
    spot = lax.broadcasted_iota(jnp.int32, (ROWS, BLK), 0)
    index_ref[...] = (spot // BLK) * ROWS + spot % BLK + at_ref[8]
    for b in range(8):
        c = at_ref[b]
        tops = got_ref[:, pl.ds(c, 1), :].reshape(8, BLK)
        own = got_ref[pl.ds(c, 1), 8:10, :].reshape(2, BLK)
        weight = own[0:1]
        target = own[1:2].astype(jnp.int32)
        top = jnp.max(tops, axis=0, keepdims=True)
        total = top + jnp.log(jnp.sum(jnp.exp(tops - top), axis=0, keepdims=True))
        total = total - jnp.log(weight)
        scores = dot(items_ref[...], users_ref[b * BLK : (b + 1) * BLK, :], (1, 1))
        share = jnp.exp(scores - total)
        dscore = jnp.where(index_ref[...] == target, share - weight, share).astype(BF16)
        all_ref[:, b * BLK : (b + 1) * BLK] = dscore
        part = dot(turned_ref[...], dscore, (1, 0))
        if b % 2 == 0:
            keep_ref[b // 2] = part
        else:
            give_ref[b // 2] = part


def user_side(at, items, users, got):
    share = jax.ShapeDtypeStruct((4, 256, BLK), F32)
    return pl.pallas_call(
        users_kernel,
        in_specs=[SMEM, VMEM, VMEM, VMEM],
        out_specs=[VMEM] * 3,
        out_shape=[jax.ShapeDtypeStruct((ROWS, ROWS), BF16), share, share],
        scratch_shapes=[pltpu.VMEM((256, ROWS), BF16), pltpu.VMEM((ROWS, BLK), jnp.int32)],
        compiler_params=pltpu.CompilerParams(vmem_limit_bytes=32 * 2**20),
        name="user_side",
    )(at, items, users, got)


def items_kernel(all_ref, users_ref, got_ref, gi_ref, ids_ref):
    ids_ref[...] = jnp.zeros_like(ids_ref)
    for z in range(8):
        if z % 2 == 0:
            pair = dot(all_ref[z * BLK : (z + 2) * BLK, :], users_ref[...], (1, 0))
        part = pair[:BLK] if z % 2 == 0 else pair[BLK:]
        largest = jnp.maximum(jnp.max(jnp.abs(part), axis=0, keepdims=True), 1e-30)
        power = jnp.ceil(jnp.log(largest) * 1.4426950408889634)
        whole = jnp.floor(part * jnp.exp2(14.9 - power) + 0.5)
        gi_ref[z, :BLK, :] = whole.astype(jnp.int32).astype(jnp.int16)
        ids_ref[z, 4:5, :] = power
    lane = lax.broadcasted_iota(jnp.int32, (8, 128), 1) // CAP
    line = lax.broadcasted_iota(jnp.int32, (8, 128), 0)
    for y in range(4):
        row = jnp.zeros((8, 128), F32)
        for p in range(8):
            piece = got_ref[p, 10 + y // 2 : 11 + y // 2, 128 * (y % 2) : 128 * (y % 2) + 128]
            piece = jnp.broadcast_to(piece, (8, 128))
            for z in range(8):
                turn = (p - z) % 8 * CAP
                row = jnp.where((lane == p) & (line == z), pltpu.roll(piece, turn, 1) if turn else piece, row)
        ids_ref[:, y, :128] = row
    gi_ref[:, BLK:, :] = ids_ref[...].astype(jnp.int32).astype(jnp.int16)


def item_side(dscore, users, got):
    return pl.pallas_call(
        items_kernel,
        in_specs=[VMEM, VMEM, VMEM],
        out_specs=VMEM,
        out_shape=jax.ShapeDtypeStruct((8, BLK + 8, 256), jnp.int16),
        scratch_shapes=[pltpu.VMEM((8, 8, 256), F32)],
        compiler_params=pltpu.CompilerParams(vmem_limit_bytes=22 * 2**20),
        name="item_side",
    )(dscore, users, got)


def tower_kernel(
    core_ref, own_ref, one_ref, two_ref, three_ref, features_ref, first_ref, second_ref,
    keep_ref, give_ref,
):
    grad_user = (own_ref[0] + one_ref[...] + two_ref[...] + three_ref[...]).astype(BF16)
    features = features_ref[...].T
    pre_act = dot(first_ref[...].T, features, (1, 0))
    hidden = jax.nn.silu(pre_act).astype(BF16)
    d_second = dot(hidden, grad_user, (1, 1))
    back_grad = dot(second_ref[...], grad_user, (1, 0))
    gate = jax.nn.sigmoid(pre_act)
    grad_pre = (back_grad * gate * (1.0 + pre_act * (1.0 - gate))).astype(BF16)
    d_first = dot(features, grad_pre, (1, 1))

    @pl.when(core_ref[0] == 0)
    def _():
        keep_ref[...] = d_first
        give_ref[...] = d_second

    @pl.when(core_ref[0] != 0)
    def _():
        keep_ref[...] = d_second
        give_ref[...] = d_first


def tower_grads(core, parts, features, w_first, w_second):
    return pl.pallas_call(
        tower_kernel,
        in_specs=[SMEM] + [VMEM] * 7,
        out_specs=[VMEM] * 2,
        out_shape=[jax.ShapeDtypeStruct((256, 256), F32)] * 2,
        compiler_params=pltpu.CompilerParams(vmem_limit_bytes=16 * 2**20),
        name="tower_grads",
    )(core, *parts, features, w_first, w_second)


def pack_kernel(parts_ref, owner_ref, rank_ref, out_ref):
    item = jnp.zeros((BLK, 256), F32)
    for z in range(8):
        power = parts_ref[z, BLK : BLK + 8, :].astype(jnp.int32).astype(F32)[4:5]
        item += parts_ref[z, :BLK, :].astype(jnp.int32).astype(F32) * jnp.exp2(power - 14.9)
    item = item.astype(BF16)
    lane = lax.broadcasted_iota(jnp.int32, (64 * 8, BLK), 0)
    halves = []
    for h in range(2):
        rank = rank_ref[...] - 8 * h
        slot = jnp.where((rank >= 0) & (rank < 8), owner_ref[...] * 8 + rank, -1)
        pick = (lane == slot).astype(F32).astype(BF16)
        halves.append(dot(pick, item, (1, 0)))
    for g in range(4):
        share = slice(64 * g, 64 * g + 64)
        both = jnp.concatenate([halves[0][:, share], halves[1][:, share]], axis=1)
        out_ref[g * 512 : (g + 1) * 512, :] = both.astype(BF16)


def pack(item, owner, rank):
    return pl.pallas_call(
        pack_kernel,
        in_specs=[VMEM] * 3,
        out_shape=jax.ShapeDtypeStruct((4 * 512, 128), BF16),
        compiler_params=pltpu.CompilerParams(vmem_limit_bytes=16 * 2**20),
        name="pack",
    )(item, owner, rank)


def table_kernel(got_ref, ids_ref, out_ref, pick_ref, kept_ref):
    both = got_ref[...].T
    value = jnp.concatenate([both[:64], both[64:]], axis=1)
    ids = ids_ref[...]
    upper = ids >> 8
    lower = ids & 255
    pick = (lax.broadcasted_iota(jnp.int32, (256, TABLE), 0) == lower).astype(F32).astype(BF16)
    pick_ref[...] = pick.T

    def step(j, carry):
        for q in range(4):
            keep = jnp.broadcast_to((upper == 4 * j + q).astype(F32), (16, TABLE)).astype(BF16)
            kept_ref[q * 64 : (q + 1) * 64, :] = value * jnp.concatenate([keep] * 4, axis=0)
        part = dot(kept_ref[...], pick_ref[...], (1, 0))
        for q in range(4):
            at = pl.multiple_of((4 * j + q) * 256, 256)
            out_ref[:, pl.ds(at, 256)] = part[q * 64 : (q + 1) * 64]
        return carry

    lax.fori_loop(0, 4, step, 0)


def table(got, ids):
    return pl.pallas_call(
        table_kernel,
        in_specs=[VMEM] * 2,
        out_shape=jax.ShapeDtypeStruct((64, TABLE), F32),
        scratch_shapes=[pltpu.VMEM((TABLE, 256), BF16), pltpu.VMEM((256, TABLE), BF16)],
        compiler_params=pltpu.CompilerParams(vmem_limit_bytes=28 * 2**20),
        name="table",
    )(got, ids)


def tower(features, w_first, w_second):
    pre_act = jnp.dot(features, w_first, preferred_element_type=F32)
    hidden = jax.nn.silu(pre_act).astype(BF16)
    return pre_act, hidden, jnp.dot(hidden, w_second, preferred_element_type=F32).astype(BF16)


def step_body(
    user_features, w_first, w_second, item_embed, example_weight, positive, item_owner, item_row
):
    features = user_features[0]
    owner = item_owner.reshape(1, BLK)
    items = to_all(item_embed[0], "z").reshape(ROWS, 256)
    pair = jnp.concatenate([features, shifted(features, "k", 1)], axis=0)
    block = jnp.concatenate([pair] + [shifted(pair, "x", d) for d in range(1, 4)], axis=0)
    _, _, users = tower(block, w_first, w_second)
    block_no = jnp.arange(8, dtype=jnp.int32)
    source = 2 * ((lax.axis_index("x") - block_no // 2) & 3) + ((block_no % 2) ^ lax.axis_index("k"))
    own_place = lax.axis_index(XK).reshape(1)
    at = jnp.concatenate([source, own_place * BLK]).astype(jnp.int32)

    member = (owner == lax.broadcasted_iota(jnp.int32, (64, 1), 0)).astype(F32)
    order = lax.broadcasted_iota(jnp.int32, (BLK, BLK), 0) < lax.broadcasted_iota(jnp.int32, (BLK, BLK), 1)
    before = dot(member.astype(BF16), order.astype(BF16), (1, 0))
    rank = jnp.sum(before * member, axis=0, keepdims=True).astype(jnp.int32)
    slot = owner * CAP + rank
    held = (slot == lax.broadcasted_iota(jnp.int32, (64 * CAP, 1), 0)).astype(jnp.int32)
    rows = jnp.sum(held * (item_row + 1), axis=1).astype(F32).reshape(64, CAP)
    rows = joined(rows, "y")
    rows = rows.reshape(4, 8, 8, CAP).transpose(2, 0, 1, 3).reshape(8, 2, BLK)
    own = jnp.concatenate([example_weight, positive.astype(F32)], axis=0)
    own = jnp.concatenate(
        [jnp.broadcast_to(own[None], (8, 2, BLK)), rows, jnp.zeros((8, 4, BLK), F32)], axis=1
    )
    got = exchange(stats(at, items, users, own), XK)
    dscore, keep, give = user_side(at, items, users, got)
    swapped = shifted(give, "k", 1)
    gi = item_side(dscore, users, got)
    gi = exchange(gi, "z")
    gu = keep + swapped
    parts = [gu] + [shifted(gu[d], "x", -d) for d in range(1, 4)]
    gu = keep + swapped
    parts = [gu] + [shifted(gu[d], "x", -d) for d in range(1, 4)]
    scale = jnp.exp2(gi[:, BLK + 4, 0].astype(F32) - 15.0)
    item = sum(gi[z, :BLK].astype(F32) * scale[z] for z in range(8)).astype(BF16)
    ids = gi[:, BLK : BLK + 4, :128].astype(jnp.int32) - 1
    ids = ids.swapaxes(0, 1).reshape(4 * 64, CAP)
    ids = jnp.concatenate([ids[:, :8].reshape(1, -1), ids[:, 8:].reshape(1, -1)], axis=1)

    core = lax.axis_index("k").astype(jnp.int32).reshape(1)
    both, other = tower_grads(core, parts, features, w_first, w_second)
    both = both + shifted(other, "k", 1)
    both = summed_share(both, "y")
    both = summed_share(both, "x")
    for step in (1, 2, 7):
        both = both + lax.ppermute(both, "z", [(i, i ^ step) for i in range(8)])

    send = pack(gi, owner, rank).reshape(256, 8, 128)
    came = exchange(send, YZXK).reshape(256 * 8, 128)
    both = to_all(both, YX).reshape(256, 256)
    grad_table = table(came, ids).T
    other = shifted(both, "k", 1)
    first = lax.axis_index("k") == 0
    return jnp.where(first, both, other), jnp.where(first, other, both), grad_table


def solution(mesh):
    torus = Mesh(mesh.devices.reshape(8, 4, 2, mesh.shape["grp"]), ("z", "x", "k", "y"))
    rows = ("z", "x", "k")
    placed = (
        P("y", rows, None),
        P(),
        P(),
        P("y", rows, None),
        P("y", rows),
        P("y", rows),
        P("y", rows, None),
        P("y", rows),
    )
    return jax.shard_map(
        step_body, mesh=torus, in_specs=placed, out_specs=(P(), P(), P(rows, "y")), check_vma=False
    )
```
